32 devices in a mesh: dp: 2 (over x), expert: 16 (over z, y, core).
Axes of the slice: x: 2, y: 2, z: 4, core: 2. Of those that a mesh axis runs over, the one named last changes fastest.
Arguments:
- tokens: bfloat16 [4096, 512], P(('dp', 'expert')), may hold values from -6 to 6
- cotangent: bfloat16 [4096, 512], P(('dp', 'expert')), may hold values from -0.29882812 to 0.29882812
- labels: int32 [4096, 1], P(('dp', 'expert')), may hold values from 0 to 31; in each aligned block of 128 rows (0 to 127, 128 to 255, ...) at most 4 rows name the same one
- placement: int32 [32], replicated, may hold values from 0 to 31, each once
- mass: float32 [4096], P(('dp', 'expert')), may hold values from 0.1 to 10
- w_head: float32 [512, 16], replicated, may hold values from -0.25 to 0.25
- w_up: bfloat16 [32, 512, 2048], P('expert', None, 'dp'), may hold values from -0.25 to 0.25
- w_down: bfloat16 [32, 2048, 512], P('expert', 'dp'), may hold values from -0.125 to 0.125
- up_moment: bfloat16 [32, 512, 2048], P('expert', None, 'dp'), may hold values from -2 to 2
- up_square: bfloat16 [32, 512, 2048], P('expert', None, 'dp'), may hold values from 0.0099487305 to 1
- down_moment: bfloat16 [32, 2048, 512], P('expert', 'dp'), may hold values from -2 to 2
- down_square: bfloat16 [32, 2048, 512], P('expert', 'dp'), may hold values from 0.0099487305 to 1
Outputs:
- fine_precip: float32 [4096, 16], P(('dp', 'expert'))
- up_next: bfloat16 [32, 512, 2048], P('expert', None, 'dp')
- down_next: bfloat16 [32, 2048, 512], P('expert', 'dp')
- up_moment_next: bfloat16 [32, 512, 2048], P('expert', None, 'dp')
- up_square_next: bfloat16 [32, 512, 2048], P('expert', None, 'dp')
- down_moment_next: bfloat16 [32, 2048, 512], P('expert', 'dp')
- down_square_next: bfloat16 [32, 2048, 512], P('expert', 'dp')
The draws below stay inside these ranges and needn't reach their ends.
Inputs may be any that keep to these rules, and one draw needn't show every extreme that they name: `labels`: within each device's block of 128 rows no regime is named more than 4 times, and in every draw some regime is named exactly 4 times in some block; every regime is named somewhere. `placement`: each regime stands in exactly one expert slot.
All inputs are finite; a program needn't handle non-finite values.
Results may differ from the reference program's by a relative error of at most 0.0045.
Values may be sent and summed in bfloat16 or wider, within the bound.
No kernel may reach another device: no remote copies, remote signals or barrier semaphores. Data moves between devices by JAX's collectives and lax.ppermute only.
A program may use at most 64 MiB of HBM per device.

```python
import math
import jax
import jax.numpy as jnp
import numpy as np
from jax import lax

D = 512
FF = 2048
PIX = 16
CAP = 4
TOK_DEV = 128
EXPERTS = 32
TOKENS = 4096
N_DP = 2
N_EXPERT = 16


def levels(rng, dims, split, smallest, largest):
    gain, own = 1.0, jax.random.fold_in(rng, 6)
    for dim, parts in split:
        heights = jnp.exp(jax.random.uniform(jax.random.fold_in(own, dim), (parts,), jnp.float32, smallest / len(split), largest / len(split)))
        gain = gain * jnp.repeat(heights, dims[dim] // parts).reshape([-1 if axis == dim else 1 for axis in range(len(dims))])
    return gain


def routed_block(rng, own, number, rows, number_of, top, reach, skew):
    ranking = jax.random.permutation(rng, number_of)
    packed, common = portions_of(number_of, rows * top, reach, skew, True), portions_of(number_of, rows * top, reach, skew, False)
    places = jnp.arange(number_of)

    def named(sizes, rotation):
        used = int((sizes > 0).sum())
        fixed = max(1, used // 4)
        moved = fixed + (places - fixed + rotation * (used - fixed)) % max(1, number_of - fixed)
        return jnp.zeros((number_of,), jnp.int32).at[ranking[jnp.where(places < fixed, places, moved)]].set(jnp.asarray(sizes, jnp.int32))

    sizes = jnp.where(number % 4 == 0, named(packed, number // 4), named(common, number - number // 4 - 1))
    mixed = jax.random.permutation(jax.random.fold_in(own, 3), number_of)
    source_of, taker = mixed[0:number_of // 2 * 2:2], mixed[1:number_of // 2 * 2:2]
    room = jnp.minimum(sizes[source_of] - 1, reach - sizes[taker]) // 2
    room = jnp.where((source_of == ranking[0]) | (taker == ranking[0]) | (sizes[taker] == 0), 0, jnp.maximum(room, 0))
    moved = jax.random.randint(jax.random.fold_in(own, 4), (number_of // 2,), 0, 1 << 20) % (room + 1)
    sizes = sizes.at[source_of].add(-moved).at[taker].add(moved)
    members = jnp.searchsorted(jnp.cumsum(sizes), jnp.arange(rows * top), side="right").astype(jnp.int32)
    table = members.reshape(top, rows).T
    table = table[jax.random.permutation(jax.random.fold_in(own, 1), rows)]
    rotation = jax.random.randint(jax.random.fold_in(own, 2), (rows, 1), 0, top)
    return jnp.take_along_axis(table, (jnp.arange(top)[None, :] + rotation) % top, axis=1)


def portions_of(count, total, reach, skew, full):
    portions = [(1 << 20) // math.isqrt(grade ** skew) + 1 for grade in range(1, count + 1)]
    largest = reach if full else min(reach, max(-(-total // count), total * portions[0] // sum(portions)))
    least = 1 if total - largest >= count - 1 else 0
    counts, spare = [largest] + [least] * (count - 1), total - largest - least * (count - 1)
    while spare > 0:
        candidates = [i for i in range(1, count) if counts[i] < largest] or [i for i in range(1, count) if counts[i] < reach]
        pool, remaining = sum([portions[i] for i in candidates]), spare
        for i in candidates:
            more = min(reach - counts[i], max(1, remaining * portions[i] // pool), spare)
            counts[i] = counts[i] + more
            spare = spare - more
    return np.array(counts)


def gaussian(own_key, dims, deviation, reach, cuts=(), held_as=jnp.bfloat16):
    result = jax.random.normal(own_key, dims, jnp.float32) * deviation
    if len(cuts) > 0:
        result = levels(own_key, dims, cuts, -0.22, 0.18) * result
    return jnp.clip(result, min=-reach, max=reach).astype(held_as)


def setup_inputs(seed: int = 0) -> dict:
    splits = jax.random.split(jax.random.key(seed), 13)
    tokens = gaussian(splits[0], (TOKENS, D), 1.0, 6.0, ((0, 32),))
    cotangent = gaussian(splits[1], (TOKENS, D), 0.05, 0.29882812, ((0, 32),))
    labels_keys = jax.random.split(jax.random.fold_in(splits[2], 1), TOKENS // TOK_DEV)
    labels_turns = jax.random.permutation(jax.random.fold_in(splits[2], 3), TOKENS // TOK_DEV)
    labels = jax.vmap(lambda own, number: routed_block(jax.random.fold_in(splits[2], 2), own, number, TOK_DEV, EXPERTS, 1, CAP, 2))(labels_keys, labels_turns).reshape((TOKENS, 1))
    placement = jax.random.permutation(splits[3], EXPERTS).astype(jnp.int32)
    mass = jnp.clip(jnp.exp(math.log(10.0) - 4.6051702 * jax.random.uniform(splits[4], (TOKENS,), jnp.float32) ** levels(splits[4], (TOKENS,), ((0, 32),), -0.2, 0.2)), 0.1, 10.0)
    w_head = gaussian(splits[5], (D, PIX), D ** -0.5, 0.25, (), jnp.float32)
    w_up = gaussian(splits[6], (EXPERTS, D, FF), D ** -0.5, 0.25, ((0, 16), (2, 2)))
    w_down = gaussian(splits[7], (EXPERTS, FF, D), FF ** -0.5, 0.125, ((0, 16), (1, 2)))
    up_moment = gaussian(splits[8], (EXPERTS, D, FF), 0.3, 2.0, ((0, 16), (2, 2)))
    up_square = jnp.clip(jnp.exp(math.log(1.0) - 4.61031033 * jax.random.uniform(splits[9], (EXPERTS, D, FF), jnp.float32) ** levels(splits[9], (EXPERTS, D, FF), ((0, 16), (2, 2)), -0.2, 0.2)), 0.0099487305, 1.0).astype(jnp.bfloat16)
    down_moment = gaussian(splits[10], (EXPERTS, FF, D), 0.3, 2.0, ((0, 16), (1, 2)))
    down_square = jnp.clip(jnp.exp(math.log(1.0) - 4.61031033 * jax.random.uniform(splits[11], (EXPERTS, FF, D), jnp.float32) ** levels(splits[11], (EXPERTS, FF, D), ((0, 16), (1, 2)), -0.2, 0.2)), 0.0099487305, 1.0).astype(jnp.bfloat16)
    return {"tokens": tokens, "cotangent": cotangent, "labels": labels, "placement": placement, "mass": mass, "w_head": w_head, "w_up": w_up, "w_down": w_down, "up_moment": up_moment, "up_square": up_square, "down_moment": down_moment, "down_square": down_square}


beta_first = 0.9
beta_second = 0.95
correct_first = 1.0 - 0.9 ** 20
correct_second = 1.0 - 0.95 ** 20
learn_rate = 0.002
adam_epsilon = 1e-08

def gelu_parts(pre):
    normal_cdf = 0.5 * (1.0 + lax.erf(pre * 0.7071067811865476))
    density = jnp.exp(-0.5 * pre * pre) * 0.3989422804014327
    return (pre * normal_cdf, normal_cdf + pre * density)

def adam_step(weight, first, second, grad):
    new_first = beta_first * first.astype(jnp.float32) + (1.0 - beta_first) * grad
    new_second = beta_second * second.astype(jnp.float32) + (1.0 - beta_second) * grad * grad
    update = new_first / correct_first / (jnp.sqrt(new_second / correct_second) + adam_epsilon)
    moved = weight.astype(jnp.float32) - learn_rate * update
    return (moved.astype(jnp.bfloat16), new_first.astype(jnp.bfloat16), new_second.astype(jnp.bfloat16))

def reference(tokens, cotangent, labels, placement, mass, w_head, w_up, w_down, up_moment, up_square, down_moment, down_square):
    experts = placement.shape[0]
    total = tokens.shape[0]
    width = tokens.shape[1]
    regimes = jnp.arange(experts, dtype=jnp.int32)
    owner = lax.optimization_barrier(jnp.sum(jnp.where(placement[None, :] == regimes[:, None], regimes[None, :], 0), axis=1)).astype(jnp.int32)
    slot_of = jnp.take(owner, labels[:, 0].astype(jnp.int32), axis=0).astype(jnp.int32)
    limit = N_DP * N_EXPERT * CAP
    share = FF // N_DP
    padded_x = jnp.concatenate([tokens, jnp.zeros((1, width), jnp.bfloat16)], axis=0)
    padded_grad = jnp.concatenate([cotangent, jnp.zeros((1, width), jnp.bfloat16)], axis=0)

    def per_expert(carry, inputs):
        slot, w_in, w_out, in_first, in_second, out_first, out_second = inputs
        rows_index = jnp.nonzero(slot_of == slot, size=limit, fill_value=total)[0].astype(jnp.int32)
        x_rows = jnp.take(padded_x, rows_index, axis=0)
        grad_rows = jnp.take(padded_grad, rows_index, axis=0)
        pre = jnp.dot(x_rows, w_in, preferred_element_type=jnp.float32)
        value, slope = gelu_parts(pre)
        hidden = value.astype(jnp.bfloat16)
        summed = jnp.zeros((limit, width), jnp.float32)
        for part in range(N_DP):
            term = jnp.dot(hidden[:, part * share:(part + 1) * share], w_out[part * share:(part + 1) * share], preferred_element_type=jnp.float32)
            summed = summed + lax.optimization_barrier(term.astype(jnp.bfloat16)).astype(jnp.float32)
        out_rows = summed.astype(jnp.bfloat16)
        back = lax.dot_general(grad_rows, w_out, (((1,), (1,)), ((), ())), preferred_element_type=jnp.float32)
        hidden_grad = (back * slope).astype(jnp.bfloat16)
        grad_in = lax.dot_general(x_rows, hidden_grad, (((0,), (0,)), ((), ())), preferred_element_type=jnp.float32)
        grad_out = lax.dot_general(hidden, grad_rows, (((0,), (0,)), ((), ())), preferred_element_type=jnp.float32)
        in_next = adam_step(w_in, in_first, in_second, grad_in)
        out_next = adam_step(w_out, out_first, out_second, grad_out)
        carry = carry.at[rows_index].set(out_rows)
        return (carry, (in_next[0], out_next[0], in_next[1], in_next[2], out_next[1], out_next[2]))
    start = jnp.zeros((total + 1, width), jnp.bfloat16)
    gathered, results = lax.scan(per_expert, start, (regimes, w_up, w_down, up_moment, up_square, down_moment, down_square))
    expert_out = gathered[:total]
    field = tokens.astype(jnp.float32) + expert_out.astype(jnp.float32)
    logits = jnp.dot(field, w_head, precision=lax.Precision.HIGHEST, preferred_element_type=jnp.float32)
    positive = jax.nn.softplus(logits) + 0.1
    fine_precip = mass[:, None] * positive / lax.optimization_barrier(jnp.sum(positive, axis=1, keepdims=True))
    return (fine_precip, results[0], results[1], results[2], results[3], results[4], results[5])
```

```python
import functools
import math

import jax
import jax.numpy as jnp
from jax import lax
from jax.experimental import pallas as pl
from jax.experimental.pallas import tpu as pltpu
from jax.sharding import PartitionSpec as P

CAP = 4

beta_first = 0.9
beta_second = 0.95
correct_first = 1.0 - 0.9**20
correct_second = 1.0 - 0.95**20
learn_rate = 0.002
adam_epsilon = 1e-08

BF = jnp.bfloat16
F32 = jnp.float32
EXACT = lax.Precision.HIGHEST
VMEM = pl.BlockSpec(memory_space=pltpu.VMEM)
SMEM = pl.BlockSpec(memory_space=pltpu.SMEM)


def iota(shape, dim):
    return lax.broadcasted_iota(jnp.int32, shape, dim)


def dot(a, b, dims=((1,), (0,)), precision=None):
    return lax.dot_general(a, b, (dims, ((), ())), precision=precision, preferred_element_type=F32)


def gelu_parts(pre):
    normal_cdf = 0.5 * (1.0 + lax.erf(pre * 0.7071067811865476))
    density = jnp.exp(-0.5 * pre * pre) * 0.3989422804014327
    return (pre * normal_cdf, normal_cdf + pre * density)


def adam_step(weight, first, second, grad):
    new_first = beta_first * first.astype(F32) + (1.0 - beta_first) * grad
    new_second = beta_second * second.astype(F32) + ((1.0 - beta_second) * grad) * grad
    scaled = new_second * (1.0 / correct_second)
    root = scaled * lax.rsqrt(scaled) + adam_epsilon
    update = (new_first * (learn_rate / correct_first)) * lax.rsqrt(root * root)
    moved = weight.astype(F32) - update
    return (moved.astype(BF), new_first.astype(BF), new_second.astype(BF))


def pack_kernel(copies, labels, placement, tokens, cotangent, head, send, slot_out, own):
    experts = placement.shape[0]
    count, width = tokens.shape
    label = labels[...]
    regime = iota((experts, count), 0)
    held = jnp.zeros((experts, count), jnp.int32)
    for j in range(experts):
        held = jnp.where(regime == j, placement[j], held)
    chosen = held == label
    before = (iota((count, count), 0) < iota((count, count), 1)).astype(F32).astype(BF)
    earlier = dot(chosen.astype(F32).astype(BF), before)
    position = jnp.sum(jnp.where(chosen, earlier, 0.0), axis=0, keepdims=True).astype(jnp.int32)
    target = jnp.sum(jnp.where(chosen, regime, 0), axis=0, keepdims=True)
    slot = target * CAP + position
    slot_out[...] = slot
    rows = experts * CAP
    pick = (iota((rows, count), 0) == slot).astype(F32).astype(BF)
    x = dot(pick, tokens[...]).astype(BF)
    g = dot(pick, cotangent[...]).astype(BF)
    for part in range(copies):
        send[pl.ds(part * rows, rows), pl.ds(0, width)] = x
        send[pl.ds(part * rows, rows), pl.ds(width, width)] = g
    own[...] = dot(head[...], tokens[...].astype(F32), ((1,), (1,)), EXACT)


def unmix(local_count, expert, group):
    rows = group * CAP
    row = iota((rows, local_count * rows), 0)
    col = iota((rows, local_count * rows), 1)
    source = row // CAP * (local_count * CAP) + expert * CAP + row % CAP
    return (source == col).astype(F32).astype(BF)


def forward_kernel(local_count, group, recv, w_up, w_down, head, hidden, slope, part_out):
    expert = pl.program_id(0)
    width = w_up.shape[1]
    pixels = head.shape[0]
    lanes = local_count * CAP * pixels
    rows = group * CAP
    groups = recv.shape[0] // (rows * local_count)
    select = unmix(local_count, expert, group)
    lane = iota((rows, lanes), 1)
    mine = (lane // (CAP * pixels) == expert) & (
        lane // pixels % CAP == iota((rows, lanes), 0) % CAP
    )
    gather = (iota((group, rows), 1) // CAP == iota((group, rows), 0)).astype(F32)
    tiled_head = jnp.concatenate([head[...]] * (local_count * CAP), axis=0)

    def step(i, carry):
        span = rows * local_count
        mixed = recv[pl.ds(pl.multiple_of(i * span, span), span), pl.ds(0, width)]
        x = dot(select, mixed).astype(BF)
        value, slant = gelu_parts(dot(x, w_up[0]))
        value = value.astype(BF)
        hidden[0, pl.ds(pl.multiple_of(i * rows, rows), rows), :] = value
        slope[0, pl.ds(pl.multiple_of(i * rows, rows), rows), :] = slant
        out = dot(value, w_down[0]).astype(BF)
        logit = dot(out.astype(F32), tiled_head, ((1,), (1,)), EXACT)
        logit = dot(gather, jnp.where(mine, logit, 0.0), precision=EXACT)
        here = pl.ds(pl.multiple_of(i * group, group), group)

        @pl.when(expert == 0)
        def _():
            part_out[here, :] = logit

        @pl.when(expert > 0)
        def _():
            part_out[here, :] += logit

        return carry

    if groups == 1:
        step(0, 0)
    else:
        lax.fori_loop(0, groups, step, 0)


def update_kernel(
    local_count,
    group,
    recv,
    hidden,
    slope,
    w_up,
    w_down,
    up_m,
    up_v,
    down_m,
    down_v,
    up_next,
    down_next,
    up_m_next,
    up_v_next,
    down_m_next,
    down_v_next,
    x_t,
    g_all,
):
    expert = pl.program_id(0)
    width = w_up.shape[1]
    chunk = w_up.shape[2]
    rows = group * CAP
    span = rows * local_count
    groups = recv.shape[0] // span

    @pl.when(pl.program_id(1) == 0)
    def _():
        select = unmix(local_count, expert, group)

        def step(i, carry):
            mixed = recv[pl.ds(pl.multiple_of(i * span, span), span), :]
            both = dot(select, mixed)
            here = pl.ds(pl.multiple_of(i * rows, rows), rows)
            x_t[:, here] = both[:, :width].T.astype(BF)
            g_all[here, :] = both[:, width:].astype(BF)
            return carry

        if groups == 1:
            step(0, 0)
        else:
            lax.fori_loop(0, groups, step, 0)

    g = g_all[...]
    back = dot(g, w_down[0], ((1,), (1,)))
    hidden_grad = (back * slope[0]).astype(BF)
    hidden_t = hidden[0].T
    tile = min(64, chunk)
    for start in range(0, width, tile):
        here = pl.ds(start, tile)
        grad = dot(x_t[here, :], hidden_grad)
        w, m, v = adam_step(w_up[0, here, :], up_m[0, here, :], up_v[0, here, :], grad)
        up_next[0, here, :] = w
        up_m_next[0, here, :] = m
        up_v_next[0, here, :] = v
    tile = min(32, chunk)
    for start in range(0, chunk, tile):
        here = pl.ds(start, tile)
        grad = dot(hidden_t[start : start + tile, :], g)
        w, m, v = adam_step(w_down[0, here, :], down_m[0, here, :], down_v[0, here, :], grad)
        down_next[0, here, :] = w
        down_m_next[0, here, :] = m
        down_v_next[0, here, :] = v


def finish_kernel(holders, slot, returned, own, mass, out):
    pixels, count = own.shape
    lanes = returned.shape[1]
    copies = returned.shape[0] // holders
    total = returned[pl.ds(0, holders), :]
    for part in range(1, copies):
        total = total + returned[pl.ds(part * holders, holders), :]
    places = lanes // pixels
    holder = slot[...] // places
    place = slot[...] % places
    pick = (iota((holders, count), 0) == holder).astype(F32)
    spread = dot(total, pick, ((0,), (0,)), EXACT)
    logits = own[...]
    for q in range(places):
        logits = logits + jnp.where(place == q, spread[q * pixels : (q + 1) * pixels, :], 0.0)
    positive = jax.nn.softplus(logits) + 0.1
    out[...] = mass[...] * positive / jnp.sum(positive, axis=0, keepdims=True)


def shape(*args):
    return jax.ShapeDtypeStruct(*args)


def local(
    tokens,
    cotangent,
    labels,
    placement,
    mass,
    w_head,
    w_up,
    w_down,
    up_moment,
    up_square,
    down_moment,
    down_square,
):
    experts = placement.shape[0]
    count, width = tokens.shape
    pixels = w_head.shape[1]
    local_count, _, hidden_count = w_up.shape
    holders = lax.axis_size("expert")
    copies = lax.axis_size("dp")
    sources = holders * copies
    group = math.gcd(sources, 32)
    lanes = local_count * CAP * pixels
    rows = sources * CAP
    mixed_rows = rows * local_count
    head = w_head.T
    axes = ("dp", "expert")

    send, slot, own = pl.pallas_call(
        functools.partial(pack_kernel, copies),
        out_shape=(
            shape((copies * experts * CAP, 2 * width), BF),
            shape((1, count), jnp.int32),
            shape((pixels, count), F32),
        ),
        in_specs=[VMEM, SMEM, VMEM, VMEM, VMEM],
        out_specs=(VMEM, VMEM, VMEM),
        name="pack",
    )(labels.reshape(1, count), placement, tokens, cotangent, head)

    recv = lax.all_to_all(send, axes, split_axis=0, concat_axis=0, tiled=True)

    hidden, slope, part_out = pl.pallas_call(
        functools.partial(forward_kernel, local_count, group),
        grid=(local_count,),
        out_shape=(
            shape((local_count, rows, hidden_count), BF),
            shape((local_count, rows, hidden_count), F32),
            shape((sources, lanes), F32),
        ),
        in_specs=[
            pl.BlockSpec((mixed_rows, width), lambda k: (0, 0)),
            pl.BlockSpec((1, width, hidden_count), lambda k: (k, 0, 0)),
            pl.BlockSpec((1, hidden_count, width), lambda k: (k, 0, 0)),
            pl.BlockSpec((pixels, width), lambda k: (0, 0)),
        ],
        out_specs=(
            pl.BlockSpec((1, rows, hidden_count), lambda k: (k, 0, 0)),
            pl.BlockSpec((1, rows, hidden_count), lambda k: (k, 0, 0)),
            pl.BlockSpec((sources, lanes), lambda k: (0, 0)),
        ),
        name="forward",
    )(recv, w_up, w_down, head)

    returned = lax.all_to_all(
        part_out.reshape(sources, 1, lanes), axes, split_axis=0, concat_axis=0, tiled=True
    ).reshape(sources, lanes)

    chunk = math.gcd(hidden_count, 256)
    up_block = pl.BlockSpec((1, width, chunk), lambda k, f: (k, 0, f))
    down_block = pl.BlockSpec((1, chunk, width), lambda k, f: (k, f, 0))
    row_block = pl.BlockSpec((1, rows, chunk), lambda k, f: (k, 0, f))
    up_shape = shape(w_up.shape, BF)
    down_shape = shape(w_down.shape, BF)
    updates = pl.pallas_call(
        functools.partial(update_kernel, local_count, group),
        grid=(local_count, hidden_count // chunk),
        out_shape=(up_shape, down_shape, up_shape, up_shape, down_shape, down_shape),
        in_specs=[
            pl.BlockSpec((mixed_rows, 2 * width), lambda k, f: (0, 0)),
            row_block,
            row_block,
            up_block,
            down_block,
            up_block,
            up_block,
            down_block,
            down_block,
        ],
        out_specs=(up_block, down_block, up_block, up_block, down_block, down_block),
        scratch_shapes=[pltpu.VMEM((width, rows), BF), pltpu.VMEM((rows, width), BF)],
        cost_estimate=pl.CostEstimate(
            flops=6 * rows * width * hidden_count * local_count,
            bytes_accessed=24 * width * hidden_count * local_count,
            transcendentals=0,
        ),
        name="update",
    )(recv, hidden, slope, w_up, w_down, up_moment, up_square, down_moment, down_square)

    fine = pl.pallas_call(
        functools.partial(finish_kernel, holders),
        out_shape=shape((pixels, count), F32),
        in_specs=[VMEM] * 4,
        out_specs=VMEM,
        name="finish",
    )(slot, returned, own, mass.reshape(1, count))
    return (fine.T,) + tuple(updates)


def solution(mesh):
    tokens = P(("dp", "expert"), None)
    up = P("expert", None, "dp")
    down = P("expert", "dp", None)
    return jax.shard_map(
        local,
        mesh=mesh,
        in_specs=(tokens, tokens, tokens, P(), P(("dp", "expert")), P())
        + (up, down, up, up, down, down),
        out_specs=(tokens, up, down, up, up, down, down),
        check_vma=False,
    )
```

```python
import functools
import math

import jax
import jax.numpy as jnp
from jax import lax
from jax.experimental import pallas as pl
from jax.experimental.pallas import tpu as pltpu
from jax.sharding import PartitionSpec as P

CAP = 4

beta_first = 0.9
beta_second = 0.95
correct_first = 1.0 - 0.9**20
correct_second = 1.0 - 0.95**20
learn_rate = 0.002
adam_epsilon = 1e-08

BF = jnp.bfloat16
F32 = jnp.float32
EXACT = lax.Precision.HIGHEST
VMEM = pl.BlockSpec(memory_space=pltpu.VMEM)
SMEM = pl.BlockSpec(memory_space=pltpu.SMEM)
HBM = pl.BlockSpec(memory_space=pltpu.HBM)


def iota(shape, dim):
    return lax.broadcasted_iota(jnp.int32, shape, dim)


def dot(a, b, dims=((1,), (0,)), precision=None):
    return lax.dot_general(a, b, (dims, ((), ())), precision=precision, preferred_element_type=F32)


def gelu_parts(pre):
    normal_cdf = 0.5 * (1.0 + lax.erf(pre * 0.7071067811865476))
    density = jnp.exp(-0.5 * pre * pre) * 0.3989422804014327
    return (pre * normal_cdf, normal_cdf + pre * density)


def adam_step(weight, first, second, grad):
    new_first = beta_first * first.astype(F32) + (1.0 - beta_first) * grad
    new_second = beta_second * second.astype(F32) + ((1.0 - beta_second) * grad) * grad
    scaled = new_second * (1.0 / correct_second)
    root = scaled * lax.rsqrt(scaled) + adam_epsilon
    update = (new_first * (learn_rate / correct_first)) * lax.rsqrt(root * root)
    moved = weight.astype(F32) - update
    return (moved.astype(BF), new_first.astype(BF), new_second.astype(BF))


def pack_kernel(labels, placement, tokens, cotangent, head, send, slot_out, own):
    experts = placement.shape[0]
    count, width = tokens.shape
    label = labels[...]
    regime = iota((experts, count), 0)
    held = jnp.zeros((experts, count), jnp.int32)
    for j in range(experts):
        held = jnp.where(regime == j, placement[j], held)
    chosen = held == label
    before = (iota((count, count), 0) < iota((count, count), 1)).astype(F32).astype(BF)
    earlier = dot(chosen.astype(F32).astype(BF), before)
    position = jnp.sum(jnp.where(chosen, earlier, 0.0), axis=0, keepdims=True).astype(jnp.int32)
    target = jnp.sum(jnp.where(chosen, regime, 0), axis=0, keepdims=True)
    slot = target * CAP + position
    slot_out[...] = slot
    pick = (iota((experts * CAP, count), 0) == slot).astype(F32).astype(BF)
    send[:, pl.ds(0, width)] = dot(pick, tokens[...]).astype(BF)
    send[:, pl.ds(width, width)] = dot(pick, cotangent[...]).astype(BF)
    own[...] = dot(head[...], tokens[...].astype(F32), ((1,), (1,)), EXACT)


def unmix(local_count, expert, rows):
    row = iota((rows, local_count * rows), 0)
    col = iota((rows, local_count * rows), 1)
    source = row // CAP * (local_count * CAP) + expert * CAP + row % CAP
    return (source == col).astype(F32).astype(BF)


def forward_rows(expert, mixed, w_up, w_down, tiled_head, pixels):
    local_count = w_up.shape[0]
    rows = mixed.shape[0] // local_count
    group = rows // CAP
    lanes = local_count * CAP * pixels
    x = dot(unmix(local_count, expert, rows), mixed).astype(BF)
    value, slant = gelu_parts(dot(x, w_up[expert]))
    value = value.astype(BF)
    out = dot(value, w_down[expert]).astype(BF)
    logit = dot(out.astype(F32), tiled_head, ((1,), (1,)), EXACT)
    lane = iota((rows, lanes), 1)
    mine = (lane // (CAP * pixels) == expert) & (
        lane // pixels % CAP == iota((rows, lanes), 0) % CAP
    )
    gather = (iota((group, rows), 1) // CAP == iota((group, rows), 0)).astype(F32)
    return value, slant, dot(gather, jnp.where(mine, logit, 0.0), precision=EXACT)


def own_kernel(recv, w_up, w_down, head, hidden, slope, part, up_here, down_here, sems):
    local_count, width, _ = w_up.shape
    copies = []
    for expert in range(local_count):
        for side, (there, here) in enumerate(((w_up, up_here), (w_down, down_here))):
            copy = pltpu.make_async_copy(
                there.at[expert], here.at[expert], sems.at[expert, side]
            )
            copy.start()
            copies.append(copy)
    tiled_head = jnp.concatenate([head[...]] * (local_count * CAP), axis=0)
    total = None
    for expert in range(local_count):
        copies[2 * expert].wait()
        copies[2 * expert + 1].wait()
        value, slant, logit = forward_rows(
            expert, recv[:, :width], up_here, down_here, tiled_head, head.shape[0]
        )
        hidden[expert] = value
        slope[expert] = slant
        total = logit if total is None else total + logit
    part[...] = total


def peer_kernel(copies, peers, w_up, w_down, head, part, hidden, slope, out):
    local_count = w_up.shape[0]
    span = peers.shape[0] // (copies - 1)
    rows = span // local_count
    group = rows // CAP
    here = lax.axis_index("dp")
    tiled_head = jnp.concatenate([head[...]] * (local_count * CAP), axis=0)
    out[pl.ds(pl.multiple_of(here * group, 8), group), :] = part[...]
    for step in range(1, copies):
        total = None
        for expert in range(local_count):
            value, slant, logit = forward_rows(
                expert,
                peers[pl.ds((step - 1) * span, span), :],
                w_up,
                w_down,
                tiled_head,
                head.shape[0],
            )
            hidden[expert, pl.ds((step - 1) * rows, rows), :] = value
            slope[expert, pl.ds((step - 1) * rows, rows), :] = slant
            total = logit if total is None else total + logit
        owner = lax.rem(here - step + copies, copies)
        out[pl.ds(pl.multiple_of(owner * group, 8), group), :] = total


def update_kernel(
    copies,
    recv,
    peer_x,
    peer_g,
    hidden_own,
    hidden_peer,
    slope_own,
    slope_peer,
    w_up,
    w_down,
    up_m,
    up_v,
    down_m,
    down_v,
    up_next,
    down_next,
    up_m_next,
    up_v_next,
    down_m_next,
    down_v_next,
    ups,
    downs,
    x_t,
    g_all,
    hidden_grad,
    hidden_t,
    sems,
):
    local_count, width, hidden_count = w_up.shape
    up_tile = math.gcd(width, 128)
    down_tile = math.gcd(hidden_count, 256)
    up_steps = width // up_tile
    down_steps = hidden_count // down_tile
    steps = up_steps + down_steps
    span = recv.shape[0]
    rows = span // local_count

    def moves(expert, step, down, out):
        tile = down_tile if down else up_tile
        held = downs if down else ups
        pairs = (
            ((w_down, down_next), (down_m, down_m_next), (down_v, down_v_next))
            if down
            else ((w_up, up_next), (up_m, up_m_next), (up_v, up_v_next))
        )
        number = expert * steps + step + (0 if down else down_steps)
        here = pl.ds(pl.multiple_of(step * tile, tile), tile)
        return [
            pltpu.make_async_copy(
                held.at[i, expert, here] if out else pair[0].at[expert, here],
                pair[1].at[expert, here] if out else held.at[i, expert, here],
                sems.at[int(out), number, i],
            )
            for i, pair in enumerate(pairs)
        ]

    def every(action, out):
        def expert_loop(expert, carry):
            for down, count in ((True, down_steps), (False, up_steps)):

                def step_loop(step, carry, down=down):
                    for move in moves(expert, step, down, out):
                        action(move)
                    return carry

                lax.fori_loop(0, count, step_loop, 0)
            return carry

        lax.fori_loop(0, local_count, expert_loop, 0)

    every(lambda move: move.start(), False)

    def expert_loop(expert, carry):
        select = unmix(local_count, expert, rows)
        for step in range(copies):
            if step == 0:
                x, g = recv[:, :width], recv[:, width:]
            else:
                x = peer_x[pl.ds((step - 1) * span, span), :]
                g = peer_g[pl.ds((step - 1) * span, span), :]
            here = pl.ds(step * rows, rows)
            x_t[:, here] = dot(select, x).T.astype(BF)
            g_all[here, :] = dot(select, g).astype(BF)
        hidden_t[:, pl.ds(0, rows)] = hidden_own[expert].T
        hidden_t[:, pl.ds(rows, rows * (copies - 1))] = hidden_peer[expert].T

        def down_loop(step, carry):
            for move in moves(expert, step, True, False):
                move.wait()
            here = pl.ds(pl.multiple_of(step * down_tile, down_tile), down_tile)
            back = dot(g_all[...], downs[0, expert, here], ((1,), (1,)))
            hidden_grad[pl.ds(0, rows), here] = (
                back[:rows] * slope_own[expert, :, here]
            ).astype(BF)
            hidden_grad[pl.ds(rows, rows * (copies - 1)), here] = (
                back[rows:] * slope_peer[expert, :, here]
            ).astype(BF)
            tile = math.gcd(down_tile, 32)
            for start in range(0, down_tile, tile):
                at = pl.ds(pl.multiple_of(step * down_tile + start, tile), tile)
                grad = dot(hidden_t[at, :], g_all[...])
                new = adam_step(*[downs[i, expert, at] for i in range(3)], grad)
                for i in range(3):
                    downs[i, expert, at] = new[i]
            for move in moves(expert, step, True, True):
                move.start()
            return carry

        lax.fori_loop(0, down_steps, down_loop, 0)

        def up_loop(step, carry):
            for move in moves(expert, step, False, False):
                move.wait()
            tile = math.gcd(up_tile, 16)
            for start in range(0, up_tile, tile):
                at = pl.ds(pl.multiple_of(step * up_tile + start, tile), tile)
                grad = dot(x_t[at, :], hidden_grad[...])
                new = adam_step(*[ups[i, expert, at] for i in range(3)], grad)
                for i in range(3):
                    ups[i, expert, at] = new[i]
            for move in moves(expert, step, False, True):
                move.start()
            return carry

        lax.fori_loop(0, up_steps, up_loop, 0)
        return carry

    lax.fori_loop(0, local_count, expert_loop, 0)
    every(lambda move: move.wait(), True)


def finish_kernel(holders, slot, returned, own, mass, out):
    pixels, count = own.shape
    lanes = returned.shape[1]
    copies = returned.shape[0] // holders
    total = returned[pl.ds(0, holders), :]
    for part in range(1, copies):
        total = total + returned[pl.ds(part * holders, holders), :]
    places = lanes // pixels
    holder = slot[...] // places
    place = slot[...] % places
    pick = (iota((holders, count), 0) == holder).astype(F32)
    spread = dot(total, pick, ((0,), (0,)), EXACT)
    logits = own[...]
    for q in range(places):
        logits = logits + jnp.where(place == q, spread[q * pixels : (q + 1) * pixels, :], 0.0)
    positive = jax.nn.softplus(logits) + 0.1
    out[...] = mass[...] * positive / jnp.sum(positive, axis=0, keepdims=True)


def shape(*args):
    return jax.ShapeDtypeStruct(*args)


def stay(value):
    return pltpu.with_memory_space_constraint(value, pltpu.HBM)


def limit(mib):
    return pltpu.CompilerParams(vmem_limit_bytes=mib << 20)


def local(
    tokens,
    cotangent,
    labels,
    placement,
    mass,
    w_head,
    w_up,
    w_down,
    up_moment,
    up_square,
    down_moment,
    down_square,
):
    w_up, w_down, up_moment, up_square, down_moment, down_square = [
        stay(value) for value in (w_up, w_down, up_moment, up_square, down_moment, down_square)
    ]
    experts = placement.shape[0]
    count, width = tokens.shape
    pixels = w_head.shape[1]
    local_count, _, hidden_count = w_up.shape
    holders = lax.axis_size("expert")
    copies = lax.axis_size("dp")
    sources = holders * copies
    lanes = local_count * CAP * pixels
    rows = holders * CAP
    head = w_head.T
    up_shape = shape(w_up.shape, BF)
    down_shape = shape(w_down.shape, BF)
    one_product = 2 * rows * width * hidden_count * local_count

    send, slot, own = pl.pallas_call(
        pack_kernel,
        out_shape=(
            shape((experts * CAP, 2 * width), BF),
            shape((1, count), jnp.int32),
            shape((pixels, count), F32),
        ),
        in_specs=[VMEM, SMEM, VMEM, VMEM, VMEM],
        out_specs=(VMEM, VMEM, VMEM),
        compiler_params=limit(4),
        name="pack",
    )(stay(labels.reshape(1, count)), stay(placement), stay(tokens), stay(cotangent), stay(head))

    recv = lax.all_to_all(send, "expert", split_axis=0, concat_axis=0, tiled=True)

    def to_peers(value):
        moved = [
            lax.ppermute(value, "dp", [(i, (i + step) % copies) for i in range(copies)])
            for step in range(1, copies)
        ]
        return moved[0] if copies == 2 else jnp.concatenate(moved, axis=0)

    peer_x = to_peers(recv[:, :width])
    peer_g = to_peers(recv[:, width:])

    hidden_own, slope_own, part, up_here, down_here = pl.pallas_call(
        own_kernel,
        out_shape=(
            shape((local_count, rows, hidden_count), BF),
            shape((local_count, rows, hidden_count), F32),
            shape((holders, lanes), F32),
            pltpu.VMEM(w_up.shape, BF),
            pltpu.VMEM(w_down.shape, BF),
        ),
        in_specs=[VMEM, HBM, HBM, VMEM],
        out_specs=(VMEM,) * 5,
        scratch_shapes=[pltpu.SemaphoreType.DMA((local_count, 2))],
        compiler_params=limit(16),
        cost_estimate=pl.CostEstimate(
            flops=4 * one_product, bytes_accessed=4 * width * hidden_count * local_count, transcendentals=0
        ),
        name="own_rows",
    )(recv, w_up, w_down, stay(head))

    hidden_peer, slope_peer, scores = pl.pallas_call(
        functools.partial(peer_kernel, copies),
        out_shape=(
            shape((local_count, rows * (copies - 1), hidden_count), BF),
            shape((local_count, rows * (copies - 1), hidden_count), F32),
            shape((sources, lanes), F32),
        ),
        in_specs=[VMEM] * 5,
        out_specs=(VMEM,) * 3,
        compiler_params=limit(16),
        cost_estimate=pl.CostEstimate(
            flops=2 * one_product, bytes_accessed=0, transcendentals=0
        ),
        name="peer_rows",
    )(peer_x, up_here, down_here, stay(head), part)

    returned = lax.all_to_all(
        scores.reshape(sources, 1, lanes),
        ("dp", "expert"),
        split_axis=0,
        concat_axis=0,
        tiled=True,
    ).reshape(sources, lanes)

    steps = width // math.gcd(width, 128) + hidden_count // math.gcd(hidden_count, 256)
    updates = pl.pallas_call(
        functools.partial(update_kernel, copies),
        out_shape=(up_shape, down_shape, up_shape, up_shape, down_shape, down_shape),
        in_specs=[VMEM] * 7 + [HBM] * 6,
        out_specs=(HBM,) * 6,
        scratch_shapes=[
            pltpu.VMEM((3,) + w_up.shape, BF),
            pltpu.VMEM((3,) + w_down.shape, BF),
            pltpu.VMEM((width, rows * copies), BF),
            pltpu.VMEM((rows * copies, width), BF),
            pltpu.VMEM((rows * copies, hidden_count), BF),
            pltpu.VMEM((hidden_count, rows * copies), BF),
            pltpu.SemaphoreType.DMA((2, local_count * steps, 3)),
        ],
        compiler_params=limit(24),
        cost_estimate=pl.CostEstimate(
            flops=6 * one_product * copies,
            bytes_accessed=24 * width * hidden_count * local_count,
            transcendentals=0,
        ),
        name="update",
    )(
        recv,
        peer_x,
        peer_g,
        hidden_own,
        hidden_peer,
        slope_own,
        slope_peer,
        w_up,
        w_down,
        up_moment,
        up_square,
        down_moment,
        down_square,
    )

    fine = pl.pallas_call(
        functools.partial(finish_kernel, holders),
        out_shape=shape((pixels, count), F32),
        in_specs=[VMEM] * 4,
        out_specs=VMEM,
        compiler_params=limit(2),
        name="finish",
    )(slot, returned, own, stay(mass.reshape(1, count)))
    return (fine.T,) + tuple(updates)


def solution(mesh):
    tokens = P(("dp", "expert"), None)
    up = P("expert", None, "dp")
    down = P("expert", "dp", None)
    return jax.shard_map(
        local,
        mesh=mesh,
        in_specs=(tokens, tokens, tokens, P(), P(("dp", "expert")), P())
        + (up, down, up, up, down, down),
        out_specs=(tokens, up, down, up, up, down, down),
        check_vma=False,
    )
```

```python
import functools
import math

import jax
import jax.numpy as jnp
from jax import lax
from jax.experimental import pallas as pl
from jax.experimental.pallas import tpu as pltpu
from jax.sharding import PartitionSpec as P

CAP = 4

beta_first = 0.9
beta_second = 0.95
correct_first = 1.0 - 0.9**20
correct_second = 1.0 - 0.95**20
learn_rate = 0.002
adam_epsilon = 1e-08

BF = jnp.bfloat16
F32 = jnp.float32
EXACT = lax.Precision.HIGHEST
VMEM = pl.BlockSpec(memory_space=pltpu.VMEM)
SMEM = pl.BlockSpec(memory_space=pltpu.SMEM)
HBM = pl.BlockSpec(memory_space=pltpu.HBM)


def iota(shape, dim):
    return lax.broadcasted_iota(jnp.int32, shape, dim)


def dot(a, b, dims=((1,), (0,)), precision=None):
    return lax.dot_general(a, b, (dims, ((), ())), precision=precision, preferred_element_type=F32)


def gelu_parts(pre):
    normal_cdf = 0.5 * (1.0 + lax.erf(pre * 0.7071067811865476))
    density = jnp.exp(-0.5 * pre * pre) * 0.3989422804014327
    return (pre * normal_cdf, normal_cdf + pre * density)


def adam_step(weight, first, second, grad):
    new_first = beta_first * first.astype(F32) + (1.0 - beta_first) * grad
    new_second = beta_second * second.astype(F32) + ((1.0 - beta_second) * grad) * grad
    root = new_second * lax.rsqrt(new_second) + adam_epsilon * correct_second**0.5
    rate = learn_rate * correct_second**0.5 / correct_first
    update = (new_first * rate) * lax.rsqrt(root * root)
    moved = weight.astype(F32) - update
    return (moved.astype(BF), new_first.astype(BF), new_second.astype(BF))


def pack_kernel(labels, placement, tokens, cotangent, head, send, slot_out, own):
    experts = placement.shape[0]
    count, width = tokens.shape
    label = labels[...]
    regime = iota((experts, count), 0)
    held = jnp.zeros((experts, count), jnp.int32)
    for j in range(experts):
        held = jnp.where(regime == j, placement[j], held)
    chosen = held == label
    before = (iota((count, count), 0) < iota((count, count), 1)).astype(F32).astype(BF)
    earlier = dot(chosen.astype(F32).astype(BF), before)
    position = jnp.sum(jnp.where(chosen, earlier, 0.0), axis=0, keepdims=True).astype(jnp.int32)
    target = jnp.sum(jnp.where(chosen, regime, 0), axis=0, keepdims=True)
    slot = target * CAP + position
    slot_out[...] = slot
    pick = (iota((experts * CAP, count), 0) == slot).astype(F32).astype(BF)
    send[:, pl.ds(0, width)] = dot(pick, tokens[...]).astype(BF)
    send[:, pl.ds(width, width)] = dot(pick, cotangent[...]).astype(BF)
    own[...] = dot(head[...], tokens[...].astype(F32), ((1,), (1,)), EXACT)


def unmix(local_count, span):
    group = span // (local_count * CAP)
    row = iota((span, span), 0)
    source = row % group * (local_count * CAP) + row // group
    return (source == iota((span, span), 1)).astype(F32).astype(BF)


def forward_rows(expert, x, w_up, w_down, heads, local_count):
    group = x.shape[0] // CAP
    lanes = heads.shape[2]
    value, slant = gelu_parts(dot(x, w_up[expert]))
    value = value.astype(BF)
    out = dot(value, w_down[expert]).astype(BF)
    logit = dot(out, heads[0]) + dot(out, heads[1]) + dot(out, heads[2])
    place = iota((group, lanes), 1) // (lanes // (local_count * CAP))
    total = jnp.zeros((group, lanes), F32)
    for c in range(CAP):
        mine = place == expert * CAP + c
        total = jnp.where(mine, logit[c * group : (c + 1) * group], total)
    return value, slant, total


def own_kernel(
    recv, w_up, w_down, head, x_own, g_own, hidden, slope, part, heads, up_here, down_here, sems
):
    local_count, width, _ = w_up.shape
    copies = []
    for expert in range(local_count):
        for side, (there, here) in enumerate(((w_up, up_here), (w_down, down_here))):
            copy = pltpu.make_async_copy(there.at[expert], here.at[expert], sems.at[expert, side])
            copy.start()
            copies.append(copy)
    span = recv.shape[0]
    rows = span // local_count
    both = dot(unmix(local_count, span), recv[...]).astype(BF)
    for expert in range(local_count):
        x_own[expert] = both[expert * rows : (expert + 1) * rows, :width]
        g_own[expert] = both[expert * rows : (expert + 1) * rows, width:]
    tiled = jnp.concatenate([head[...]] * (local_count * CAP), axis=0).T
    for i in range(3):
        piece = tiled.astype(BF)
        heads[i] = piece
        tiled = tiled - piece.astype(F32)
    total = None
    for expert in range(local_count):
        copies[2 * expert].wait()
        copies[2 * expert + 1].wait()
        value, slant, logit = forward_rows(
            expert, x_own[expert], up_here, down_here, heads, local_count
        )
        hidden[expert] = value
        slope[expert] = slant
        total = logit if total is None else total + logit
    part[...] = total


def peer_kernel(copies, peers, w_up, w_down, heads, part, x_peer, hidden, slope, out):
    local_count = w_up.shape[0]
    span = peers.shape[0] // (copies - 1)
    rows = span // local_count
    group = rows // CAP
    here = lax.axis_index("dp")
    select = unmix(local_count, span)
    out[pl.ds(pl.multiple_of(here * group, 8), group), :] = part[...]
    for step in range(1, copies):
        at = pl.ds((step - 1) * rows, rows)
        x = dot(select, peers[pl.ds((step - 1) * span, span), :]).astype(BF)
        total = None
        for expert in range(local_count):
            mine = x[expert * rows : (expert + 1) * rows]
            x_peer[expert, at, :] = mine
            value, slant, logit = forward_rows(expert, mine, w_up, w_down, heads, local_count)
            hidden[expert, at, :] = value
            slope[expert, at, :] = slant
            total = logit if total is None else total + logit
        owner = lax.rem(here - step + copies, copies)
        out[pl.ds(pl.multiple_of(owner * group, 8), group), :] = total


def update_kernel(
    copies,
    x_own,
    x_peer,
    g_own,
    peer_g,
    hidden_own,
    hidden_peer,
    slope_own,
    slope_peer,
    w_up,
    w_down,
    up_m,
    up_v,
    down_m,
    down_v,
    up_next,
    down_next,
    up_m_next,
    up_v_next,
    down_m_next,
    down_v_next,
    ups,
    downs,
    x_t,
    g_all,
    hidden_grad,
    up_grad,
    down_grad,
    sems,
):
    local_count, width, hidden_count = w_up.shape
    up_tile = up_grad.shape[1]
    down_tile = down_grad.shape[1]
    blocks = []
    for expert in range(local_count):
        blocks += [(expert, True, step) for step in range(hidden_count // down_tile)]
        blocks += [(expert, False, step) for step in range(width // up_tile)]

    def moves(number, out):
        expert, down, step = blocks[number]
        tile, held = (down_tile, downs) if down else (up_tile, ups)
        pairs = (
            ((w_down, down_next), (down_m, down_m_next), (down_v, down_v_next))
            if down
            else ((w_up, up_next), (up_m, up_m_next), (up_v, up_v_next))
        )
        here = pl.ds(step * tile, tile)
        return [
            pltpu.make_async_copy(
                held.at[i, expert, here] if out else pair[0].at[expert, here],
                pair[1].at[expert, here] if out else held.at[i, expert, here],
                sems.at[int(out), number, i],
            )
            for i, pair in enumerate(pairs)
        ]

    for number in range(len(blocks)):
        for move in moves(number, False):
            move.start()

    span = peer_g.shape[0] // (copies - 1)
    rows = span // local_count
    select = unmix(local_count, span)
    for step in range(1, copies):
        g = dot(select, peer_g[pl.ds((step - 1) * span, span), :]).astype(BF)
        for expert in range(local_count):
            g_all[expert, pl.ds(step * rows, rows), :] = g[expert * rows : (expert + 1) * rows]
    for expert in range(local_count):
        g_all[expert, pl.ds(0, rows), :] = g_own[expert]
        x_t[expert] = jnp.concatenate([x_own[expert], x_peer[expert]], axis=0).T

    def stage(number):
        expert, down, step = blocks[number]
        if down:
            here = pl.ds(step * down_tile, down_tile)
            back = dot(g_all[expert], downs[0, expert, here], ((1,), (1,)))
            slope = jnp.concatenate([slope_own[expert, :, here], slope_peer[expert, :, here]], axis=0)
            hidden_grad[expert, :, here] = (back * slope).astype(BF)
            hidden = jnp.concatenate([hidden_own[expert, :, here], hidden_peer[expert, :, here]], axis=0)
            down_grad[number % 2] = dot(hidden.T, g_all[expert])
        else:
            here = pl.ds(step * up_tile, up_tile)
            up_grad[number % 2] = dot(x_t[expert, here, :], hidden_grad[expert])

    def settle(number):
        expert, down, step = blocks[number]
        held, grads = (downs, down_grad) if down else (ups, up_grad)
        count = grads.shape[1]
        tile = math.gcd(count, 32 if down else 16)
        for start in range(0, count, tile):
            at = pl.ds(step * count + start, tile)
            new = adam_step(
                *[held[i, expert, at] for i in range(3)], grads[number % 2, pl.ds(start, tile)]
            )
            for i in range(3):
                held[i, expert, at] = new[i]

    for move in moves(0, False):
        move.wait()
    stage(0)
    for number in range(len(blocks)):
        if number + 1 < len(blocks):
            for move in moves(number + 1, False):
                move.wait()
            stage(number + 1)
        settle(number)
        for move in moves(number, True):
            move.start()
    for number in range(len(blocks)):
        for move in moves(number, True):
            move.wait()


def finish_kernel(holders, slot, returned, own, mass, out):
    pixels, count = own.shape
    lanes = returned.shape[1]
    copies = returned.shape[0] // holders
    total = returned[pl.ds(0, holders), :]
    for part in range(1, copies):
        total = total + returned[pl.ds(part * holders, holders), :]
    places = lanes // pixels
    holder = slot[...] // places
    place = slot[...] % places
    pick = (iota((holders, count), 0) == holder).astype(F32)
    spread = dot(total, pick, ((0,), (0,)), EXACT)
    logits = own[...]
    for q in range(places):
        logits = logits + jnp.where(place == q, spread[q * pixels : (q + 1) * pixels, :], 0.0)
    positive = jax.nn.softplus(logits) + 0.1
    out[...] = mass[...] * positive / jnp.sum(positive, axis=0, keepdims=True)


def shape(*args):
    return jax.ShapeDtypeStruct(*args)


def stay(value):
    return pltpu.with_memory_space_constraint(value, pltpu.HBM)


def limit(mib):
    return pltpu.CompilerParams(vmem_limit_bytes=mib << 20)


def local(
    tokens,
    cotangent,
    labels,
    placement,
    mass,
    w_head,
    w_up,
    w_down,
    up_moment,
    up_square,
    down_moment,
    down_square,
):
    w_up, w_down, up_moment, up_square, down_moment, down_square = [
        stay(value) for value in (w_up, w_down, up_moment, up_square, down_moment, down_square)
    ]
    experts = placement.shape[0]
    count, width = tokens.shape
    pixels = w_head.shape[1]
    local_count, _, hidden_count = w_up.shape
    holders = lax.axis_size("expert")
    copies = lax.axis_size("dp")
    sources = holders * copies
    lanes = local_count * CAP * pixels
    rows = holders * CAP
    head = w_head.T
    up_shape = shape(w_up.shape, BF)
    down_shape = shape(w_down.shape, BF)
    one_product = 2 * rows * width * hidden_count * local_count

    send, slot, own = pl.pallas_call(
        pack_kernel,
        out_shape=(
            shape((experts * CAP, 2 * width), BF),
            shape((1, count), jnp.int32),
            shape((pixels, count), F32),
        ),
        in_specs=[VMEM, SMEM, VMEM, VMEM, VMEM],
        out_specs=(VMEM, VMEM, VMEM),
        compiler_params=limit(4),
        name="pack",
    )(stay(labels.reshape(1, count)), stay(placement), stay(tokens), stay(cotangent), stay(head))

    recv = lax.all_to_all(send, "expert", split_axis=0, concat_axis=0, tiled=True)

    def to_peers(value):
        moved = [
            lax.ppermute(value, "dp", [(i, (i + step) % copies) for i in range(copies)])
            for step in range(1, copies)
        ]
        return moved[0] if copies == 2 else jnp.concatenate(moved, axis=0)

    peer_x = to_peers(recv[:, :width])
    peer_g = to_peers(recv[:, width:])

    x_own, g_own, hidden_own, slope_own, part, heads, up_here, down_here = pl.pallas_call(
        own_kernel,
        out_shape=(
            shape((local_count, rows, width), BF),
            shape((local_count, rows, width), BF),
            shape((local_count, rows, hidden_count), BF),
            shape((local_count, rows, hidden_count), F32),
            shape((holders, lanes), F32),
            pltpu.VMEM((3, width, lanes), BF),
            pltpu.VMEM(w_up.shape, BF),
            pltpu.VMEM(w_down.shape, BF),
        ),
        in_specs=[VMEM, HBM, HBM, VMEM],
        out_specs=(VMEM,) * 8,
        scratch_shapes=[pltpu.SemaphoreType.DMA((local_count, 2))],
        compiler_params=limit(16),
        cost_estimate=pl.CostEstimate(
            flops=4 * one_product,
            bytes_accessed=4 * width * hidden_count * local_count,
            transcendentals=0,
        ),
        name="own_rows",
    )(recv, w_up, w_down, stay(head))

    others = rows * (copies - 1)
    x_peer, hidden_peer, slope_peer, scores = pl.pallas_call(
        functools.partial(peer_kernel, copies),
        out_shape=(
            shape((local_count, others, width), BF),
            shape((local_count, others, hidden_count), BF),
            shape((local_count, others, hidden_count), F32),
            shape((sources, lanes), F32),
        ),
        in_specs=[VMEM] * 5,
        out_specs=(VMEM,) * 4,
        compiler_params=limit(16),
        cost_estimate=pl.CostEstimate(flops=2 * one_product, bytes_accessed=0, transcendentals=0),
        name="peer_rows",
    )(peer_x, up_here, down_here, heads, part)

    returned = lax.all_to_all(
        scores.reshape(sources, 1, lanes),
        ("dp", "expert"),
        split_axis=0,
        concat_axis=0,
        tiled=True,
    ).reshape(sources, lanes)

    up_tile = math.gcd(width, 128)
    down_tile = math.gcd(hidden_count, 256)
    blocks = local_count * (width // up_tile + hidden_count // down_tile)
    updates = pl.pallas_call(
        functools.partial(update_kernel, copies),
        out_shape=(up_shape, down_shape, up_shape, up_shape, down_shape, down_shape),
        in_specs=[VMEM] * 8 + [HBM] * 6,
        out_specs=(HBM,) * 6,
        scratch_shapes=[
            pltpu.VMEM((3,) + w_up.shape, BF),
            pltpu.VMEM((3,) + w_down.shape, BF),
            pltpu.VMEM((local_count, width, rows * copies), BF),
            pltpu.VMEM((local_count, rows * copies, width), BF),
            pltpu.VMEM((local_count, rows * copies, hidden_count), BF),
            pltpu.VMEM((2, up_tile, hidden_count), F32),
            pltpu.VMEM((2, down_tile, width), F32),
            pltpu.SemaphoreType.DMA((2, blocks, 3)),
        ],
        compiler_params=limit(28),
        cost_estimate=pl.CostEstimate(
            flops=6 * one_product * copies,
            bytes_accessed=24 * width * hidden_count * local_count,
            transcendentals=0,
        ),
        name="update",
    )(
        x_own,
        x_peer,
        g_own,
        peer_g,
        hidden_own,
        hidden_peer,
        slope_own,
        slope_peer,
        w_up,
        w_down,
        up_moment,
        up_square,
        down_moment,
        down_square,
    )

    fine = pl.pallas_call(
        functools.partial(finish_kernel, holders),
        out_shape=shape((pixels, count), F32),
        in_specs=[VMEM] * 4,
        out_specs=VMEM,
        compiler_params=limit(2),
        name="finish",
    )(slot, returned, own, mass.reshape(1, count))
    return (fine.T,) + tuple(updates)


def solution(mesh):
    tokens = P(("dp", "expert"), None)
    up = P("expert", None, "dp")
    down = P("expert", "dp", None)
    return jax.shard_map(
        local,
        mesh=mesh,
        in_specs=(tokens, tokens, tokens, P(), P(("dp", "expert")), P())
        + (up, down, up, up, down, down),
        out_specs=(tokens, up, down, up, up, down, down),
        check_vma=False,
    )
```

```python
import functools
import math

import jax
import jax.numpy as jnp
from jax import lax
from jax.experimental import pallas as pl
from jax.experimental.pallas import tpu as pltpu
from jax.sharding import PartitionSpec as P

CAP = 4
AHEAD = 2.0

beta_first = 0.9
beta_second = 0.95
correct_first = 1.0 - 0.9**20
correct_second = 1.0 - 0.95**20
learn_rate = 0.002
adam_epsilon = 1e-08

BF = jnp.bfloat16
F32 = jnp.float32
EXACT = lax.Precision.HIGHEST
VMEM = pl.BlockSpec(memory_space=pltpu.VMEM)
SMEM = pl.BlockSpec(memory_space=pltpu.SMEM)
HBM = pl.BlockSpec(memory_space=pltpu.HBM)


def iota(shape, dim):
    return lax.broadcasted_iota(jnp.int32, shape, dim)


def dot(a, b, dims=((1,), (0,)), precision=None):
    return lax.dot_general(a, b, (dims, ((), ())), precision=precision, preferred_element_type=F32)


def gelu_parts(pre):
    normal_cdf = 0.5 * (1.0 + lax.erf(pre * 0.7071067811865476))
    density = jnp.exp(-0.5 * pre * pre) * 0.3989422804014327
    return (pre * normal_cdf, normal_cdf + pre * density)


def adam_step(weight, first, second, grad):
    new_first = beta_first * first.astype(F32) + (1.0 - beta_first) * grad
    new_second = beta_second * second.astype(F32) + ((1.0 - beta_second) * grad) * grad
    root = new_second * lax.rsqrt(new_second) + adam_epsilon * correct_second**0.5
    rate = learn_rate * correct_second**0.5 / correct_first
    update = (new_first * rate) * lax.rsqrt(root * root)
    moved = weight.astype(F32) - update
    return (moved.astype(BF), new_first.astype(BF), new_second.astype(BF))


def pack_kernel(labels, placement, tokens, cotangent, send, slot_out):
    experts = placement.shape[0]
    count, width = tokens.shape
    label = labels[...]
    regime = iota((experts, count), 0)
    held = jnp.zeros((experts, count), jnp.int32)
    for j in range(experts):
        held = jnp.where(regime == j, placement[j], held)
    chosen = held == label
    before = (iota((count, count), 0) < iota((count, count), 1)).astype(F32).astype(BF)
    earlier = dot(chosen.astype(F32).astype(BF), before)
    position = jnp.sum(jnp.where(chosen, earlier, 0.0), axis=0, keepdims=True).astype(jnp.int32)
    target = jnp.sum(jnp.where(chosen, regime, 0), axis=0, keepdims=True)
    slot = target * CAP + position
    slot_out[...] = slot
    pick = (iota((experts * CAP, count), 0) == slot).astype(F32).astype(BF)
    send[:, pl.ds(0, width)] = dot(pick, tokens[...]).astype(BF)
    send[:, pl.ds(width, width)] = dot(pick, cotangent[...]).astype(BF)


def unmix(local_count, span):
    group = span // (local_count * CAP)
    row = iota((span, span), 0)
    source = row % group * (local_count * CAP) + row // group
    return (source == iota((span, span), 1)).astype(F32).astype(BF)


def score_rows(expert, value, w_down, heads, local_count):
    group = value.shape[0] // CAP
    lanes = heads.shape[2]
    out = dot(value, w_down).astype(BF)
    logit = dot(out, heads[0]) + dot(out, heads[1]) + dot(out, heads[2])
    place = iota((group, lanes), 1) // (lanes // (local_count * CAP))
    total = jnp.zeros((group, lanes), F32)
    for c in range(CAP):
        mine = place == expert * CAP + c
        total = jnp.where(mine, logit[c * group : (c + 1) * group], total)
    return total


def own_kernel(
    recv,
    w_up,
    w_down,
    head,
    tokens,
    x_own,
    g_own,
    hidden,
    slope,
    part,
    heads,
    own,
    up_here,
    down_first,
    down_rest,
    head_here,
    tokens_here,
    sems,
    small_sems,
):
    local_count, width, _ = w_up.shape
    small = [
        pltpu.make_async_copy(head, head_here, small_sems.at[0]),
        pltpu.make_async_copy(tokens, tokens_here, small_sems.at[1]),
    ]
    for copy in small:
        copy.start()
    copies = []
    for side in range(2):
        for expert in range(local_count):
            if side == 0:
                there, here = w_up.at[expert], up_here.at[expert]
            else:
                there = w_down.at[expert]
                here = down_rest.at[expert - 1] if expert else down_first
            copy = pltpu.make_async_copy(there, here, sems.at[expert, side])
            copy.start()
            copies.append(copy)
    span = recv.shape[0]
    rows = span // local_count
    both = dot(unmix(local_count, span), recv[...]).astype(BF)
    for expert in range(local_count):
        x_own[expert] = both[expert * rows : (expert + 1) * rows, :width]
        g_own[expert] = both[expert * rows : (expert + 1) * rows, width:]
    for copy in small:
        copy.wait()
    rest = jnp.concatenate([head_here[...]] * (local_count * CAP), axis=0).T
    for i in range(3):
        piece = rest.astype(BF)
        heads[i] = piece
        rest = rest - piece.astype(F32)
    own[...] = dot(head_here[...], tokens_here[...].astype(F32), ((1,), (1,)), EXACT)
    for expert in range(local_count):
        copies[expert].wait()
        value, slant = gelu_parts(dot(x_own[expert], up_here[expert]))
        hidden[expert] = value.astype(BF)
        slope[expert] = slant
    total = None
    for expert in range(local_count):
        copies[local_count + expert].wait()
        weight = down_rest[expert - 1] if expert else down_first[...]
        logit = score_rows(expert, hidden[expert], weight, heads, local_count)
        total = logit if total is None else total + logit
    part[...] = total


def peer_kernel(
    copies, peers, w_up, down_first, down_rest, heads, part, x_peer, hidden, slope, out
):
    local_count = w_up.shape[0]
    span = peers.shape[0] // (copies - 1)
    rows = span // local_count
    group = rows // CAP
    here = lax.axis_index("dp")
    select = unmix(local_count, span)
    out[pl.ds(pl.multiple_of(here * group, 8), group), :] = part[...]
    for step in range(1, copies):
        at = pl.ds((step - 1) * rows, rows)
        x = dot(select, peers[pl.ds((step - 1) * span, span), :]).astype(BF)
        total = None
        for expert in range(local_count):
            mine = x[expert * rows : (expert + 1) * rows]
            x_peer[expert, at, :] = mine
            value, slant = gelu_parts(dot(mine, w_up[expert]))
            value = value.astype(BF)
            hidden[expert, at, :] = value
            weight = down_rest[expert - 1] if expert else down_first[...]
            logit = score_rows(expert, value, weight, heads, local_count)
            slope[expert, at, :] = slant
            total = logit if total is None else total + logit
        owner = lax.rem(here - step + copies, copies)
        out[pl.ds(pl.multiple_of(owner * group, 8), group), :] = total


def graded(total, small_first, small_last):
    if total % 128:
        return [total]
    sizes = [total // 8, total // 8, total // 4, total // 2] if small_first else [total // 2] * 2
    if small_last:
        sizes = [total // 2, total // 4, total // 8, total // 8]
    return sizes


def update_blocks(local_count, width, hidden_count):
    blocks = []
    for expert in range(local_count):
        for down in (True, False):
            start = 0
            first = expert == 0 and down
            last = expert == local_count - 1 and not down
            for size in graded(hidden_count if down else width, first, last):
                blocks.append((expert, down, start, size))
                start += size
    return blocks


def update_kernel(
    copies,
    x_own,
    x_peer,
    g_own,
    peer_g,
    hidden_own,
    hidden_peer,
    slope_own,
    slope_peer,
    w_up,
    w_down,
    up_m,
    up_v,
    down_m,
    down_v,
    up_next,
    down_next,
    up_m_next,
    up_v_next,
    down_m_next,
    down_v_next,
    ups,
    downs,
    x_t,
    g_all,
    hidden_grad,
    up_grad,
    down_grad,
    sems,
):
    local_count, width, hidden_count = w_up.shape
    blocks = update_blocks(local_count, width, hidden_count)

    def block_rows(block):
        return block[3] * (width if block[1] else hidden_count) / (width * hidden_count)

    def moves(number, out):
        expert, down, start, size = blocks[number]
        held = downs if down else ups
        pairs = (
            ((w_down, down_next), (down_m, down_m_next), (down_v, down_v_next))
            if down
            else ((w_up, up_next), (up_m, up_m_next), (up_v, up_v_next))
        )
        here = pl.ds(start, size)
        return [
            pltpu.make_async_copy(
                held.at[i, expert, here] if out else pair[0].at[expert, here],
                pair[1].at[expert, here] if out else held.at[i, expert, here],
                sems.at[int(out), number, i],
            )
            for i, pair in enumerate(pairs)
        ]

    due = []
    asked = 0
    for number in range(len(blocks) + 1):
        due.append([])
        done = sum(block_rows(block) for block in blocks[:number])
        while asked < len(blocks) and (
            asked <= number or sum(block_rows(block) for block in blocks[: asked + 1]) - done <= AHEAD
        ):
            due[number].append(asked)
            asked += 1

    for other in due[0]:
        for move in moves(other, False):
            move.start()

    span = peer_g.shape[0] // (copies - 1)
    rows = span // local_count
    select = unmix(local_count, span)
    for step in range(1, copies):
        g = dot(select, peer_g[pl.ds((step - 1) * span, span), :]).astype(BF)
        for expert in range(local_count):
            g_all[expert, pl.ds(step * rows, rows), :] = g[expert * rows : (expert + 1) * rows]
    for expert in range(local_count):
        g_all[expert, pl.ds(0, rows), :] = g_own[expert]
        x_t[expert] = jnp.concatenate([x_own[expert], x_peer[expert]], axis=0).T

    def stage(number):
        expert, down, start, size = blocks[number]
        if down:
            here = pl.ds(start, size)
            back = dot(g_all[expert], downs[0, expert, here], ((1,), (1,)))
            slope = jnp.concatenate([slope_own[expert, :, here], slope_peer[expert, :, here]], axis=0)
            hidden_grad[expert, :, here] = (back * slope).astype(BF)
            hidden = jnp.concatenate([hidden_own[expert, :, here], hidden_peer[expert, :, here]], axis=0)
            down_grad[number % 2, pl.ds(0, size)] = dot(hidden.T, g_all[expert])
        else:
            here = pl.ds(start, size)
            up_grad[number % 2, pl.ds(0, size)] = dot(x_t[expert, here, :], hidden_grad[expert])

    def settle(number):
        expert, down, start, size = blocks[number]
        held, grads = (downs, down_grad) if down else (ups, up_grad)
        tile = math.gcd(size, 32 if down else 16)
        for row in range(0, size, tile):
            at = pl.ds(start + row, tile)
            new = adam_step(
                *[held[i, expert, at] for i in range(3)], grads[number % 2, pl.ds(row, tile)]
            )
            for i in range(3):
                held[i, expert, at] = new[i]

    for move in moves(0, False):
        move.wait()
    stage(0)
    for number in range(len(blocks)):
        for other in due[number + 1]:
            for move in moves(other, False):
                move.start()
        if number + 1 < len(blocks):
            for move in moves(number + 1, False):
                move.wait()
            stage(number + 1)
        settle(number)
        for move in moves(number, True):
            move.start()
    for number in range(len(blocks)):
        for move in moves(number, True):
            move.wait()


def finish_kernel(holders, slot, returned, own, mass, out):
    pixels, count = own.shape
    lanes = returned.shape[1]
    copies = returned.shape[0] // holders
    total = returned[pl.ds(0, holders), :]
    for part in range(1, copies):
        total = total + returned[pl.ds(part * holders, holders), :]
    places = lanes // pixels
    holder = slot[...] // places
    place = slot[...] % places
    pick = (iota((holders, count), 0) == holder).astype(F32)
    spread = dot(total, pick, ((0,), (0,)), EXACT)
    logits = own[...]
    for q in range(places):
        logits = logits + jnp.where(place == q, spread[q * pixels : (q + 1) * pixels, :], 0.0)
    positive = jax.nn.softplus(logits) + 0.1
    out[...] = mass[...] * positive / jnp.sum(positive, axis=0, keepdims=True)


def shape(*args):
    return jax.ShapeDtypeStruct(*args)


def stay(value):
    return pltpu.with_memory_space_constraint(value, pltpu.HBM)


def limit(mib):
    return pltpu.CompilerParams(vmem_limit_bytes=mib << 20)


def local(
    tokens,
    cotangent,
    labels,
    placement,
    mass,
    w_head,
    w_up,
    w_down,
    up_moment,
    up_square,
    down_moment,
    down_square,
):
    w_up, w_down, up_moment, up_square, down_moment, down_square = [
        stay(value) for value in (w_up, w_down, up_moment, up_square, down_moment, down_square)
    ]
    experts = placement.shape[0]
    count, width = tokens.shape
    pixels = w_head.shape[1]
    local_count, _, hidden_count = w_up.shape
    holders = lax.axis_size("expert")
    copies = lax.axis_size("dp")
    sources = holders * copies
    lanes = local_count * CAP * pixels
    rows = holders * CAP
    head = w_head.T
    up_shape = shape(w_up.shape, BF)
    down_shape = shape(w_down.shape, BF)
    one_product = 2 * rows * width * hidden_count * local_count

    send, slot = pl.pallas_call(
        pack_kernel,
        out_shape=(
            shape((experts * CAP, 2 * width), BF),
            shape((1, count), jnp.int32),
        ),
        in_specs=[VMEM, SMEM, VMEM, VMEM],
        out_specs=(VMEM, VMEM),
        compiler_params=limit(4),
        name="pack",
    )(stay(labels.reshape(1, count)), stay(placement), stay(tokens), stay(cotangent))

    recv = lax.all_to_all(send, "expert", split_axis=0, concat_axis=0, tiled=True)

    def to_peers(value):
        moved = [
            lax.ppermute(value, "dp", [(i, (i + step) % copies) for i in range(copies)])
            for step in range(1, copies)
        ]
        return moved[0] if copies == 2 else jnp.concatenate(moved, axis=0)

    peer_x = to_peers(recv[:, :width])

    (
        x_own, g_own, hidden_own, slope_own, part, heads, own, up_here, down_first, down_rest
    ) = pl.pallas_call(
        own_kernel,
        out_shape=(
            shape((local_count, rows, width), BF),
            shape((local_count, rows, width), BF),
            shape((local_count, rows, hidden_count), BF),
            shape((local_count, rows, hidden_count), F32),
            shape((holders, lanes), F32),
            pltpu.VMEM((3, width, lanes), BF),
            shape((pixels, count), F32),
            pltpu.VMEM(w_up.shape, BF),
            pltpu.VMEM(w_down.shape[1:], BF),
            pltpu.VMEM((local_count - 1,) + w_down.shape[1:], BF),
        ),
        in_specs=[VMEM, HBM, HBM, HBM, HBM],
        out_specs=(VMEM,) * 10,
        scratch_shapes=[
            pltpu.VMEM(head.shape, F32),
            pltpu.VMEM(tokens.shape, BF),
            pltpu.SemaphoreType.DMA((local_count, 2)),
            pltpu.SemaphoreType.DMA((2,)),
        ],
        compiler_params=limit(16),
        cost_estimate=pl.CostEstimate(
            flops=4 * one_product,
            bytes_accessed=4 * width * hidden_count * local_count,
            transcendentals=0,
        ),
        name="own_rows",
    )(recv, w_up, w_down, stay(head), stay(tokens))

    peer_x, recv_g, part = lax.optimization_barrier((peer_x, recv[:, width:], part))
    peer_g = to_peers(recv_g)
    others = rows * (copies - 1)
    x_peer, hidden_peer, slope_peer, scores = pl.pallas_call(
        functools.partial(peer_kernel, copies),
        out_shape=(
            shape((local_count, others, width), BF),
            shape((local_count, others, hidden_count), BF),
            shape((local_count, others, hidden_count), F32),
            shape((sources, lanes), F32),
        ),
        in_specs=[VMEM] * 6,
        out_specs=(VMEM,) * 4,
        compiler_params=limit(16),
        cost_estimate=pl.CostEstimate(flops=2 * one_product, bytes_accessed=0, transcendentals=0),
        name="peer_rows",
    )(peer_x, up_here, down_first, down_rest, heads, part)

    returned = lax.all_to_all(
        scores.reshape(sources, 1, lanes),
        ("dp", "expert"),
        split_axis=0,
        concat_axis=0,
        tiled=True,
    ).reshape(sources, lanes)

    blocks = update_blocks(local_count, width, hidden_count)
    up_tile, down_tile = [max(b[3] for b in blocks if b[1] == down) for down in (False, True)]
    updates = pl.pallas_call(
        functools.partial(update_kernel, copies),
        out_shape=(up_shape, down_shape, up_shape, up_shape, down_shape, down_shape),
        in_specs=[VMEM] * 8 + [HBM] * 6,
        out_specs=(HBM,) * 6,
        scratch_shapes=[
            pltpu.VMEM((3,) + w_up.shape, BF),
            pltpu.VMEM((3,) + w_down.shape, BF),
            pltpu.VMEM((local_count, width, rows * copies), BF),
            pltpu.VMEM((local_count, rows * copies, width), BF),
            pltpu.VMEM((local_count, rows * copies, hidden_count), BF),
            pltpu.VMEM((2, up_tile, hidden_count), F32),
            pltpu.VMEM((2, down_tile, width), F32),
            pltpu.SemaphoreType.DMA((2, len(blocks), 3)),
        ],
        compiler_params=limit(28),
        cost_estimate=pl.CostEstimate(
            flops=6 * one_product * copies,
            bytes_accessed=24 * width * hidden_count * local_count,
            transcendentals=0,
        ),
        name="update",
    )(
        x_own,
        x_peer,
        g_own,
        peer_g,
        hidden_own,
        hidden_peer,
        slope_own,
        slope_peer,
        w_up,
        w_down,
        up_moment,
        up_square,
        down_moment,
        down_square,
    )

    returned, updates = lax.optimization_barrier((returned, updates))
    fine = pl.pallas_call(
        functools.partial(finish_kernel, holders),
        out_shape=shape((pixels, count), F32),
        in_specs=[VMEM] * 4,
        out_specs=VMEM,
        compiler_params=limit(2),
        name="finish",
    )(slot, returned, own, mass.reshape(1, count))
    return (fine.T,) + tuple(updates)


def solution(mesh):
    tokens = P(("dp", "expert"), None)
    up = P("expert", None, "dp")
    down = P("expert", "dp", None)
    return jax.shard_map(
        local,
        mesh=mesh,
        in_specs=(tokens, tokens, tokens, P(), P(("dp", "expert")), P())
        + (up, down, up, up, down, down),
        out_specs=(tokens, up, down, up, up, down, down),
        check_vma=False,
    )
```

```python
import functools
import math

import jax
import jax.numpy as jnp
from jax import lax
from jax.experimental import pallas as pl
from jax.experimental.pallas import tpu as pltpu
from jax.sharding import PartitionSpec as P

CAP = 4
AHEAD = 2.0

beta_first = 0.9
beta_second = 0.95
correct_first = 1.0 - 0.9**20
correct_second = 1.0 - 0.95**20
learn_rate = 0.002
adam_epsilon = 1e-08

BF = jnp.bfloat16
F32 = jnp.float32
EXACT = lax.Precision.HIGHEST
VMEM = pl.BlockSpec(memory_space=pltpu.VMEM)
SMEM = pl.BlockSpec(memory_space=pltpu.SMEM)
HBM = pl.BlockSpec(memory_space=pltpu.HBM)


def iota(shape, dim):
    return lax.broadcasted_iota(jnp.int32, shape, dim)


def dot(a, b, dims=((1,), (0,)), precision=None):
    return lax.dot_general(a, b, (dims, ((), ())), precision=precision, preferred_element_type=F32)


def gelu_parts(pre):
    normal_cdf = 0.5 * (1.0 + lax.erf(pre * 0.7071067811865476))
    density = jnp.exp(-0.5 * pre * pre) * 0.3989422804014327
    return (pre * normal_cdf, normal_cdf + pre * density)


def adam_step(weight, first, second, grad):
    new_first = beta_first * first.astype(F32) + (1.0 - beta_first) * grad
    new_second = beta_second * second.astype(F32) + ((1.0 - beta_second) * grad) * grad
    root = new_second * lax.rsqrt(new_second) + adam_epsilon * correct_second**0.5
    rate = learn_rate * correct_second**0.5 / correct_first
    update = (new_first * rate) * lax.rsqrt(root * root)
    moved = weight.astype(F32) - update
    return (moved.astype(BF), new_first.astype(BF), new_second.astype(BF))


def pack_kernel(labels, placement, tokens, cotangent, send, slot_out):
    experts = placement.shape[0]
    count, width = tokens.shape
    label = labels[...]
    regime = iota((experts, count), 0)
    held = jnp.zeros((experts, count), jnp.int32)
    for j in range(experts):
        held = jnp.where(regime == j, placement[j], held)
    chosen = held == label
    before = (iota((count, count), 0) < iota((count, count), 1)).astype(F32).astype(BF)
    earlier = dot(chosen.astype(F32).astype(BF), before)
    position = jnp.sum(jnp.where(chosen, earlier, 0.0), axis=0, keepdims=True).astype(jnp.int32)
    target = jnp.sum(jnp.where(chosen, regime, 0), axis=0, keepdims=True)
    slot = target * CAP + position
    slot_out[...] = slot
    pick = (iota((experts * CAP, count), 0) == slot).astype(F32).astype(BF)
    send[:, pl.ds(0, width)] = dot(pick, tokens[...]).astype(BF)
    send[:, pl.ds(width, width)] = dot(pick, cotangent[...]).astype(BF)


def unmix(local_count, span):
    group = span // (local_count * CAP)
    row = iota((span, span), 0)
    source = row % group * (local_count * CAP) + row // group
    return (source == iota((span, span), 1)).astype(F32).astype(BF)


def score_rows(expert, value, w_down, heads, local_count):
    group = value.shape[0] // CAP
    lanes = heads.shape[2]
    out = dot(value, w_down).astype(BF)
    logit = dot(out, heads[0]) + dot(out, heads[1]) + dot(out, heads[2])
    place = iota((group, lanes), 1) // (lanes // (local_count * CAP))
    total = jnp.zeros((group, lanes), F32)
    for c in range(CAP):
        mine = place == expert * CAP + c
        total = jnp.where(mine, logit[c * group : (c + 1) * group], total)
    return total


def own_kernel(
    recv,
    w_up,
    w_down,
    head,
    tokens,
    x_own,
    g_own,
    hidden,
    slope,
    part,
    heads,
    own,
    up_here,
    down_first,
    down_rest,
    head_here,
    tokens_here,
    sems,
    small_sems,
):
    local_count, width, _ = w_up.shape
    small = [
        pltpu.make_async_copy(head, head_here, small_sems.at[0]),
        pltpu.make_async_copy(tokens, tokens_here, small_sems.at[1]),
    ]
    for copy in small:
        copy.start()
    copies = []
    for side in range(2):
        for expert in range(local_count):
            if side == 0:
                there, here = w_up.at[expert], up_here.at[expert]
            else:
                there = w_down.at[expert]
                here = down_rest.at[expert - 1] if expert else down_first
            copy = pltpu.make_async_copy(there, here, sems.at[expert, side])
            copy.start()
            copies.append(copy)
    span = recv.shape[0]
    rows = span // local_count
    both = dot(unmix(local_count, span), recv[...]).astype(BF)
    for expert in range(local_count):
        x_own[expert] = both[expert * rows : (expert + 1) * rows, :width]
        g_own[expert] = both[expert * rows : (expert + 1) * rows, width:]
    for copy in small:
        copy.wait()
    rest = head_here[...]
    pieces = []
    for i in range(3):
        piece = rest.astype(BF)
        pieces.append(piece)
        heads[i] = jnp.concatenate([piece] * (local_count * CAP), axis=0).T
        rest = rest - piece.astype(F32)
    pixels = head.shape[0]
    terms = dot(jnp.concatenate(pieces, axis=0), tokens_here[...], ((1,), (1,)))
    own[...] = terms[:pixels] + terms[pixels : 2 * pixels] + terms[2 * pixels :]
    for expert in range(local_count):
        copies[expert].wait()
        value, slant = gelu_parts(dot(x_own[expert], up_here[expert]))
        hidden[expert] = value.astype(BF)
        slope[expert] = slant
    total = None
    for expert in range(local_count):
        copies[local_count + expert].wait()
        weight = down_rest[expert - 1] if expert else down_first[...]
        logit = score_rows(expert, hidden[expert], weight, heads, local_count)
        total = logit if total is None else total + logit
    part[...] = total


def peer_kernel(
    copies, peers, w_up, down_first, down_rest, heads, part, x_peer, hidden, slope, out
):
    local_count = w_up.shape[0]
    span = peers.shape[0] // (copies - 1)
    rows = span // local_count
    group = rows // CAP
    here = lax.axis_index("dp")
    select = unmix(local_count, span)
    out[pl.ds(pl.multiple_of(here * group, 8), group), :] = part[...]
    for step in range(1, copies):
        at = pl.ds((step - 1) * rows, rows)
        x = dot(select, peers[pl.ds((step - 1) * span, span), :]).astype(BF)
        total = None
        for expert in range(local_count):
            mine = x[expert * rows : (expert + 1) * rows]
            x_peer[expert, at, :] = mine
            value, slant = gelu_parts(dot(mine, w_up[expert]))
            value = value.astype(BF)
            hidden[expert, at, :] = value
            weight = down_rest[expert - 1] if expert else down_first[...]
            logit = score_rows(expert, value, weight, heads, local_count)
            slope[expert, at, :] = slant
            total = logit if total is None else total + logit
        owner = lax.rem(here - step + copies, copies)
        out[pl.ds(pl.multiple_of(owner * group, 8), group), :] = total


def graded(total, small_first, small_last):
    if total % 128:
        return [total]
    sizes = [total // 8, total // 8, total // 4, total // 2] if small_first else [total // 2] * 2
    if small_last:
        sizes = [total // 2, total // 4, total // 8, total // 8]
    return sizes


def update_blocks(local_count, width, hidden_count):
    blocks = []
    for expert in range(local_count):
        for down in (True, False):
            start = 0
            first = expert == 0 and down
            last = expert == local_count - 1 and not down
            for size in graded(hidden_count if down else width, first, last):
                blocks.append((expert, down, start, size))
                start += size
    return blocks


def update_kernel(
    copies,
    x_own,
    x_peer,
    g_own,
    peer_g,
    hidden_own,
    hidden_peer,
    slope_own,
    slope_peer,
    w_up,
    w_down,
    up_m,
    up_v,
    down_m,
    down_v,
    up_next,
    down_next,
    up_m_next,
    up_v_next,
    down_m_next,
    down_v_next,
    ups,
    downs,
    x_t,
    g_all,
    hidden_grad,
    up_grad,
    down_grad,
    sems,
):
    local_count, width, hidden_count = w_up.shape
    blocks = update_blocks(local_count, width, hidden_count)

    def block_rows(block):
        return block[3] * (width if block[1] else hidden_count) / (width * hidden_count)

    def moves(number, out):
        expert, down, start, size = blocks[number]
        held = downs if down else ups
        pairs = (
            ((w_down, down_next), (down_m, down_m_next), (down_v, down_v_next))
            if down
            else ((w_up, up_next), (up_m, up_m_next), (up_v, up_v_next))
        )
        here = pl.ds(start, size)
        return [
            pltpu.make_async_copy(
                held.at[i, expert, here] if out else pair[0].at[expert, here],
                pair[1].at[expert, here] if out else held.at[i, expert, here],
                sems.at[int(out), number, i],
            )
            for i, pair in enumerate(pairs)
        ]

    due = []
    asked = 0
    for number in range(len(blocks) + 1):
        due.append([])
        done = sum(block_rows(block) for block in blocks[:number])
        while asked < len(blocks) and (
            asked <= number or sum(block_rows(block) for block in blocks[: asked + 1]) - done <= AHEAD
        ):
            due[number].append(asked)
            asked += 1

    for other in due[0]:
        for move in moves(other, False):
            move.start()

    span = peer_g.shape[0] // (copies - 1)
    rows = span // local_count
    select = unmix(local_count, span)
    for step in range(1, copies):
        g = dot(select, peer_g[pl.ds((step - 1) * span, span), :]).astype(BF)
        for expert in range(local_count):
            g_all[expert, pl.ds(step * rows, rows), :] = g[expert * rows : (expert + 1) * rows]
    for expert in range(local_count):
        g_all[expert, pl.ds(0, rows), :] = g_own[expert]
        x_t[expert] = jnp.concatenate([x_own[expert], x_peer[expert]], axis=0).T

    def stage(number):
        expert, down, start, size = blocks[number]
        if down:
            here = pl.ds(start, size)
            back = dot(g_all[expert], downs[0, expert, here], ((1,), (1,)))
            slope = jnp.concatenate([slope_own[expert, :, here], slope_peer[expert, :, here]], axis=0)
            hidden_grad[expert, :, here] = (back * slope).astype(BF)
            hidden = jnp.concatenate([hidden_own[expert, :, here], hidden_peer[expert, :, here]], axis=0)
            down_grad[number % 2, pl.ds(0, size)] = dot(hidden.T, g_all[expert])
        else:
            here = pl.ds(start, size)
            up_grad[number % 2, pl.ds(0, size)] = dot(x_t[expert, here, :], hidden_grad[expert])

    def settle(number):
        expert, down, start, size = blocks[number]
        held, grads = (downs, down_grad) if down else (ups, up_grad)
        tile = math.gcd(size, 32 if down else 16)
        for row in range(0, size, tile):
            at = pl.ds(start + row, tile)
            new = adam_step(
                *[held[i, expert, at] for i in range(3)], grads[number % 2, pl.ds(row, tile)]
            )
            for i in range(3):
                held[i, expert, at] = new[i]

    for move in moves(0, False):
        move.wait()
    stage(0)
    for number in range(len(blocks)):
        for other in due[number + 1]:
            for move in moves(other, False):
                move.start()
        if number + 1 < len(blocks):
            for move in moves(number + 1, False):
                move.wait()
            stage(number + 1)
        settle(number)
        for move in moves(number, True):
            move.start()
    for number in range(len(blocks)):
        for move in moves(number, True):
            move.wait()


def finish_kernel(holders, slot, returned, own, mass, out):
    pixels, count = own.shape
    lanes = returned.shape[1]
    copies = returned.shape[0] // holders
    total = returned[pl.ds(0, holders), :]
    for part in range(1, copies):
        total = total + returned[pl.ds(part * holders, holders), :]
    places = lanes // pixels
    holder = slot[...] // places
    place = slot[...] % places
    pick = (iota((holders, count), 0) == holder).astype(F32)
    spread = dot(total, pick, ((0,), (0,)), EXACT)
    logits = own[...]
    for q in range(places):
        logits = logits + jnp.where(place == q, spread[q * pixels : (q + 1) * pixels, :], 0.0)
    positive = jax.nn.softplus(logits) + 0.1
    out[...] = mass[...] * positive / jnp.sum(positive, axis=0, keepdims=True)


def shape(*args):
    return jax.ShapeDtypeStruct(*args)


def stay(value):
    return pltpu.with_memory_space_constraint(value, pltpu.HBM)


def limit(mib):
    return pltpu.CompilerParams(vmem_limit_bytes=mib << 20)


def local(
    tokens,
    cotangent,
    labels,
    placement,
    mass,
    w_head,
    w_up,
    w_down,
    up_moment,
    up_square,
    down_moment,
    down_square,
):
    w_up, w_down, up_moment, up_square, down_moment, down_square = [
        stay(value) for value in (w_up, w_down, up_moment, up_square, down_moment, down_square)
    ]
    experts = placement.shape[0]
    count, width = tokens.shape
    pixels = w_head.shape[1]
    local_count, _, hidden_count = w_up.shape
    holders = lax.axis_size("expert")
    copies = lax.axis_size("dp")
    sources = holders * copies
    lanes = local_count * CAP * pixels
    rows = holders * CAP
    head = w_head.T
    up_shape = shape(w_up.shape, BF)
    down_shape = shape(w_down.shape, BF)
    one_product = 2 * rows * width * hidden_count * local_count

    send, slot = pl.pallas_call(
        pack_kernel,
        out_shape=(
            shape((experts * CAP, 2 * width), BF),
            shape((1, count), jnp.int32),
        ),
        in_specs=[VMEM, SMEM, VMEM, VMEM],
        out_specs=(VMEM, VMEM),
        compiler_params=limit(4),
        name="pack",
    )(stay(labels.reshape(1, count)), stay(placement), stay(tokens), stay(cotangent))

    recv = lax.all_to_all(send, "expert", split_axis=0, concat_axis=0, tiled=True)

    def to_peers(value):
        moved = [
            lax.ppermute(value, "dp", [(i, (i + step) % copies) for i in range(copies)])
            for step in range(1, copies)
        ]
        return moved[0] if copies == 2 else jnp.concatenate(moved, axis=0)

    peer_x = to_peers(recv[:, :width])

    (
        x_own, g_own, hidden_own, slope_own, part, heads, own, up_here, down_first, down_rest
    ) = pl.pallas_call(
        own_kernel,
        out_shape=(
            shape((local_count, rows, width), BF),
            shape((local_count, rows, width), BF),
            shape((local_count, rows, hidden_count), BF),
            shape((local_count, rows, hidden_count), F32),
            shape((holders, lanes), F32),
            pltpu.VMEM((3, width, lanes), BF),
            shape((pixels, count), F32),
            pltpu.VMEM(w_up.shape, BF),
            pltpu.VMEM(w_down.shape[1:], BF),
            pltpu.VMEM((local_count - 1,) + w_down.shape[1:], BF),
        ),
        in_specs=[VMEM, HBM, HBM, HBM, HBM],
        out_specs=(VMEM,) * 10,
        scratch_shapes=[
            pltpu.VMEM(head.shape, F32),
            pltpu.VMEM(tokens.shape, BF),
            pltpu.SemaphoreType.DMA((local_count, 2)),
            pltpu.SemaphoreType.DMA((2,)),
        ],
        compiler_params=limit(16),
        cost_estimate=pl.CostEstimate(
            flops=4 * one_product,
            bytes_accessed=4 * width * hidden_count * local_count,
            transcendentals=0,
        ),
        name="own_rows",
    )(recv, w_up, w_down, stay(head), stay(tokens))

    recv_g, part = lax.optimization_barrier((recv[:, width:], part))
    peer_g = to_peers(recv_g)
    peer_x, part = lax.optimization_barrier((peer_x, part))
    others = rows * (copies - 1)
    x_peer, hidden_peer, slope_peer, scores = pl.pallas_call(
        functools.partial(peer_kernel, copies),
        out_shape=(
            shape((local_count, others, width), BF),
            shape((local_count, others, hidden_count), BF),
            shape((local_count, others, hidden_count), F32),
            shape((sources, lanes), F32),
        ),
        in_specs=[VMEM] * 6,
        out_specs=(VMEM,) * 4,
        compiler_params=limit(16),
        cost_estimate=pl.CostEstimate(flops=2 * one_product, bytes_accessed=0, transcendentals=0),
        name="peer_rows",
    )(peer_x, up_here, down_first, down_rest, heads, part)

    returned = lax.all_to_all(
        scores.reshape(sources, 1, lanes),
        ("dp", "expert"),
        split_axis=0,
        concat_axis=0,
        tiled=True,
    ).reshape(sources, lanes)

    blocks = update_blocks(local_count, width, hidden_count)
    up_tile, down_tile = [max(b[3] for b in blocks if b[1] == down) for down in (False, True)]
    updates = pl.pallas_call(
        functools.partial(update_kernel, copies),
        out_shape=(up_shape, down_shape, up_shape, up_shape, down_shape, down_shape),
        in_specs=[VMEM] * 8 + [HBM] * 6,
        out_specs=(HBM,) * 6,
        scratch_shapes=[
            pltpu.VMEM((3,) + w_up.shape, BF),
            pltpu.VMEM((3,) + w_down.shape, BF),
            pltpu.VMEM((local_count, width, rows * copies), BF),
            pltpu.VMEM((local_count, rows * copies, width), BF),
            pltpu.VMEM((local_count, rows * copies, hidden_count), BF),
            pltpu.VMEM((2, up_tile, hidden_count), F32),
            pltpu.VMEM((2, down_tile, width), F32),
            pltpu.SemaphoreType.DMA((2, len(blocks), 3)),
        ],
        compiler_params=limit(28),
        cost_estimate=pl.CostEstimate(
            flops=6 * one_product * copies,
            bytes_accessed=24 * width * hidden_count * local_count,
            transcendentals=0,
        ),
        name="update",
    )(
        x_own,
        x_peer,
        g_own,
        peer_g,
        hidden_own,
        hidden_peer,
        slope_own,
        slope_peer,
        w_up,
        w_down,
        up_moment,
        up_square,
        down_moment,
        down_square,
    )

    returned, updates = lax.optimization_barrier((returned, updates))
    fine = pl.pallas_call(
        functools.partial(finish_kernel, holders),
        out_shape=shape((pixels, count), F32),
        in_specs=[VMEM] * 4,
        out_specs=VMEM,
        compiler_params=limit(2),
        name="finish",
    )(slot, returned, own, mass.reshape(1, count))
    return (fine.T,) + tuple(updates)


def solution(mesh):
    tokens = P(("dp", "expert"), None)
    up = P("expert", None, "dp")
    down = P("expert", "dp", None)
    return jax.shard_map(
        local,
        mesh=mesh,
        in_specs=(tokens, tokens, tokens, P(), P(("dp", "expert")), P())
        + (up, down, up, up, down, down),
        out_specs=(tokens, up, down, up, up, down, down),
        check_vma=False,
    )
```

```python
import functools
import math

import jax
import jax.numpy as jnp
from jax import lax
from jax.experimental import pallas as pl
from jax.experimental.pallas import tpu as pltpu
from jax.sharding import PartitionSpec as P

CAP = 4
AHEAD = 2.0

beta_first = 0.9
beta_second = 0.95
correct_first = 1.0 - 0.9**20
correct_second = 1.0 - 0.95**20
learn_rate = 0.002
adam_epsilon = 1e-08

BF = jnp.bfloat16
F32 = jnp.float32
EXACT = lax.Precision.HIGHEST
VMEM = pl.BlockSpec(memory_space=pltpu.VMEM)
SMEM = pl.BlockSpec(memory_space=pltpu.SMEM)
HBM = pl.BlockSpec(memory_space=pltpu.HBM)


def iota(shape, dim):
    return lax.broadcasted_iota(jnp.int32, shape, dim)


def dot(a, b, dims=((1,), (0,)), precision=None):
    return lax.dot_general(a, b, (dims, ((), ())), precision=precision, preferred_element_type=F32)


def gelu_parts(pre):
    normal_cdf = 0.5 * (1.0 + lax.erf(pre * 0.7071067811865476))
    density = jnp.exp(-0.5 * pre * pre) * 0.3989422804014327
    return (pre * normal_cdf, normal_cdf + pre * density)


def adam_step(weight, first, second, grad):
    new_first = beta_first * first.astype(F32) + (1.0 - beta_first) * grad
    new_second = beta_second * second.astype(F32) + ((1.0 - beta_second) * grad) * grad
    root = new_second * lax.rsqrt(new_second) + adam_epsilon * correct_second**0.5
    rate = learn_rate * correct_second**0.5 / correct_first
    update = (new_first * rate) * lax.rsqrt(root * root)
    moved = weight.astype(F32) - update
    return (moved.astype(BF), new_first.astype(BF), new_second.astype(BF))


def pack_kernel(labels, placement, tokens, cotangent, send, slot_out):
    experts = placement.shape[0]
    count, width = tokens.shape
    label = labels[...]
    regime = iota((experts, count), 0)
    held = jnp.zeros((experts, count), jnp.int32)
    for j in range(experts):
        held = jnp.where(regime == j, placement[j], held)
    chosen = held == label
    before = (iota((count, count), 0) < iota((count, count), 1)).astype(F32).astype(BF)
    earlier = dot(chosen.astype(F32).astype(BF), before)
    position = jnp.sum(jnp.where(chosen, earlier, 0.0), axis=0, keepdims=True).astype(jnp.int32)
    target = jnp.sum(jnp.where(chosen, regime, 0), axis=0, keepdims=True)
    slot = target * CAP + position
    slot_out[...] = slot
    pick = (iota((experts * CAP, count), 0) == slot).astype(F32).astype(BF)
    send[:, pl.ds(0, width)] = dot(pick, tokens[...]).astype(BF)
    send[:, pl.ds(width, width)] = dot(pick, cotangent[...]).astype(BF)


def unmix(local_count, span):
    group = span // (local_count * CAP)
    row = iota((span, span), 0)
    source = row % group * (local_count * CAP) + row // group
    return (source == iota((span, span), 1)).astype(F32).astype(BF)


def score_rows(expert, value, w_down, heads, local_count):
    rows = value[0].shape[0]
    group = rows // CAP
    lanes = heads.shape[2]
    out = dot(jnp.concatenate(value, axis=0), w_down).astype(BF)
    logit = dot(out, heads[0]) + dot(out, heads[1]) + dot(out, heads[2])
    place = iota((group, lanes), 1) // (lanes // (local_count * CAP))
    totals = []
    for start in range(0, rows * len(value), rows):
        total = jnp.zeros((group, lanes), F32)
        for c in range(CAP):
            mine = place == expert * CAP + c
            at = start + c * group
            total = jnp.where(mine, logit[at : at + group], total)
        totals.append(total)
    return totals


def own_kernel(
    recv,
    w_up,
    w_down,
    head,
    tokens,
    x_own,
    g_own,
    hidden,
    slope,
    heads,
    own,
    up_here,
    down_first,
    down_rest,
    head_here,
    tokens_here,
    sems,
    small_sems,
):
    local_count, width, _ = w_up.shape
    small = [
        pltpu.make_async_copy(head, head_here, small_sems.at[0]),
        pltpu.make_async_copy(tokens, tokens_here, small_sems.at[1]),
    ]
    for copy in small:
        copy.start()
    copies = []
    for side in range(2):
        for expert in range(local_count):
            if side == 0:
                there, here = w_up.at[expert], up_here.at[expert]
            else:
                there = w_down.at[expert]
                here = down_rest.at[expert - 1] if expert else down_first
            copy = pltpu.make_async_copy(there, here, sems.at[expert, side])
            copy.start()
            copies.append(copy)
    span = recv.shape[0]
    rows = span // local_count
    both = dot(unmix(local_count, span), recv[...]).astype(BF)
    for expert in range(local_count):
        x_own[expert] = both[expert * rows : (expert + 1) * rows, :width]
        g_own[expert] = both[expert * rows : (expert + 1) * rows, width:]
    for copy in small:
        copy.wait()
    rest = head_here[...]
    pieces = []
    for i in range(3):
        piece = rest.astype(BF)
        pieces.append(piece)
        heads[i] = jnp.concatenate([piece] * (local_count * CAP), axis=0).T
        rest = rest - piece.astype(F32)
    pixels = head.shape[0]
    terms = dot(jnp.concatenate(pieces, axis=0), tokens_here[...], ((1,), (1,)))
    own[...] = terms[:pixels] + terms[pixels : 2 * pixels] + terms[2 * pixels :]
    for expert in range(local_count):
        copies[expert].wait()
        value, slant = gelu_parts(dot(x_own[expert], up_here[expert]))
        hidden[expert] = value.astype(BF)
        slope[expert] = slant
    for copy in copies[local_count:]:
        copy.wait()


def peer_kernel(
    copies, peers, w_up, down_first, down_rest, heads, hidden_own, x_peer, hidden, slope, out
):
    local_count = w_up.shape[0]
    span = peers.shape[0] // (copies - 1)
    rows = span // local_count
    group = rows // CAP
    here = lax.axis_index("dp")
    select = unmix(local_count, span)
    for step in range(1, copies):
        at = pl.ds((step - 1) * rows, rows)
        x = dot(select, peers[pl.ds((step - 1) * span, span), :]).astype(BF)
        totals = None
        for expert in range(local_count):
            mine = x[expert * rows : (expert + 1) * rows]
            x_peer[expert, at, :] = mine
            value, slant = gelu_parts(dot(mine, w_up[expert]))
            value = value.astype(BF)
            hidden[expert, at, :] = value
            weight = down_rest[expert - 1] if expert else down_first[...]
            slope[expert, at, :] = slant
            values = [value, hidden_own[expert]] if step == 1 else [value]
            terms = score_rows(expert, values, weight, heads, local_count)
            totals = terms if totals is None else [a + b for a, b in zip(totals, terms)]
        owner = lax.rem(here - step + copies, copies)
        for place, total in zip((owner, here), totals):
            out[pl.ds(pl.multiple_of(place * group, 8), group), :] = total


def graded(total, small_first, small_last):
    if total % 128:
        return [total]
    sizes = [total // 8, total // 8, total // 4, total // 2] if small_first else [total // 2] * 2
    if small_last:
        sizes = [total // 2, total // 4, total // 8, total // 8]
    return sizes


def update_blocks(local_count, width, hidden_count):
    blocks = []
    for expert in range(local_count):
        for down in (True, False):
            start = 0
            first = expert == 0 and down
            last = expert == local_count - 1 and not down
            for size in graded(hidden_count if down else width, first, last):
                blocks.append((expert, down, start, size))
                start += size
    return blocks


def update_kernel(
    copies,
    x_own,
    x_peer,
    g_own,
    peer_g,
    hidden_own,
    hidden_peer,
    slope_own,
    slope_peer,
    w_up,
    w_down,
    up_m,
    up_v,
    down_m,
    down_v,
    up_next,
    down_next,
    up_m_next,
    up_v_next,
    down_m_next,
    down_v_next,
    ups,
    downs,
    x_t,
    g_all,
    hidden_grad,
    up_grad,
    down_grad,
    sems,
):
    local_count, width, hidden_count = w_up.shape
    blocks = update_blocks(local_count, width, hidden_count)

    def block_rows(block):
        return block[3] * (width if block[1] else hidden_count) / (width * hidden_count)

    def moves(number, out):
        expert, down, start, size = blocks[number]
        held = downs if down else ups
        pairs = (
            ((w_down, down_next), (down_m, down_m_next), (down_v, down_v_next))
            if down
            else ((w_up, up_next), (up_m, up_m_next), (up_v, up_v_next))
        )
        here = pl.ds(start, size)
        return [
            pltpu.make_async_copy(
                held.at[i, expert, here] if out else pair[0].at[expert, here],
                pair[1].at[expert, here] if out else held.at[i, expert, here],
                sems.at[int(out), number, i],
            )
            for i, pair in enumerate(pairs)
        ]

    due = []
    asked = 0
    for number in range(len(blocks) + 1):
        due.append([])
        done = sum(block_rows(block) for block in blocks[:number])
        while asked < len(blocks) and (
            asked <= number or sum(block_rows(block) for block in blocks[: asked + 1]) - done <= AHEAD
        ):
            due[number].append(asked)
            asked += 1

    for other in due[0]:
        for move in moves(other, False):
            move.start()

    span = peer_g.shape[0] // (copies - 1)
    rows = span // local_count
    select = unmix(local_count, span)
    for step in range(1, copies):
        g = dot(select, peer_g[pl.ds((step - 1) * span, span), :]).astype(BF)
        for expert in range(local_count):
            g_all[expert, pl.ds(step * rows, rows), :] = g[expert * rows : (expert + 1) * rows]
    for expert in range(local_count):
        g_all[expert, pl.ds(0, rows), :] = g_own[expert]
        x_t[expert] = jnp.concatenate([x_own[expert], x_peer[expert]], axis=0).T

    def stage(number):
        expert, down, start, size = blocks[number]
        if down:
            here = pl.ds(start, size)
            back = dot(g_all[expert], downs[0, expert, here], ((1,), (1,)))
            slope = jnp.concatenate([slope_own[expert, :, here], slope_peer[expert, :, here]], axis=0)
            hidden_grad[expert, :, here] = (back * slope).astype(BF)
            hidden = jnp.concatenate([hidden_own[expert, :, here], hidden_peer[expert, :, here]], axis=0)
            down_grad[number % 2, pl.ds(0, size)] = dot(hidden.T, g_all[expert])
        else:
            here = pl.ds(start, size)
            up_grad[number % 2, pl.ds(0, size)] = dot(x_t[expert, here, :], hidden_grad[expert])

    def settle(number):
        expert, down, start, size = blocks[number]
        held, grads = (downs, down_grad) if down else (ups, up_grad)
        tile = math.gcd(size, 32 if down else 16)
        for row in range(0, size, tile):
            at = pl.ds(start + row, tile)
            new = adam_step(
                *[held[i, expert, at] for i in range(3)], grads[number % 2, pl.ds(row, tile)]
            )
            for i in range(3):
                held[i, expert, at] = new[i]

    for move in moves(0, False):
        move.wait()
    stage(0)
    for number in range(len(blocks)):
        for other in due[number + 1]:
            for move in moves(other, False):
                move.start()
        if number + 1 < len(blocks):
            for move in moves(number + 1, False):
                move.wait()
            stage(number + 1)
        settle(number)
        for move in moves(number, True):
            move.start()
    for number in range(len(blocks)):
        for move in moves(number, True):
            move.wait()


def finish_kernel(holders, slot, returned, own, mass, out):
    pixels, count = own.shape
    lanes = returned.shape[1]
    copies = returned.shape[0] // holders
    total = returned[pl.ds(0, holders), :]
    for part in range(1, copies):
        total = total + returned[pl.ds(part * holders, holders), :]
    places = lanes // pixels
    holder = slot[...] // places
    place = slot[...] % places
    pick = (iota((holders, count), 0) == holder).astype(F32)
    spread = dot(total, pick, ((0,), (0,)), EXACT)
    logits = own[...]
    for q in range(places):
        logits = logits + jnp.where(place == q, spread[q * pixels : (q + 1) * pixels, :], 0.0)
    positive = jax.nn.softplus(logits) + 0.1
    out[...] = mass[...] * positive / jnp.sum(positive, axis=0, keepdims=True)


def shape(*args):
    return jax.ShapeDtypeStruct(*args)


def stay(value):
    return pltpu.with_memory_space_constraint(value, pltpu.HBM)


def limit(mib):
    return pltpu.CompilerParams(vmem_limit_bytes=mib << 20)


def local(
    tokens,
    cotangent,
    labels,
    placement,
    mass,
    w_head,
    w_up,
    w_down,
    up_moment,
    up_square,
    down_moment,
    down_square,
):
    w_up, w_down, up_moment, up_square, down_moment, down_square = [
        stay(value) for value in (w_up, w_down, up_moment, up_square, down_moment, down_square)
    ]
    experts = placement.shape[0]
    count, width = tokens.shape
    pixels = w_head.shape[1]
    local_count, _, hidden_count = w_up.shape
    holders = lax.axis_size("expert")
    copies = lax.axis_size("dp")
    sources = holders * copies
    lanes = local_count * CAP * pixels
    rows = holders * CAP
    head = w_head.T
    up_shape = shape(w_up.shape, BF)
    down_shape = shape(w_down.shape, BF)
    one_product = 2 * rows * width * hidden_count * local_count

    send, slot = pl.pallas_call(
        pack_kernel,
        out_shape=(
            shape((experts * CAP, 2 * width), BF),
            shape((1, count), jnp.int32),
        ),
        in_specs=[VMEM, SMEM, VMEM, VMEM],
        out_specs=(VMEM, VMEM),
        compiler_params=limit(4),
        name="pack",
    )(stay(labels.reshape(1, count)), stay(placement), stay(tokens), stay(cotangent))

    recv = lax.all_to_all(send, "expert", split_axis=0, concat_axis=0, tiled=True)

    def to_peers(value):
        moved = [
            lax.ppermute(value, "dp", [(i, (i + step) % copies) for i in range(copies)])
            for step in range(1, copies)
        ]
        return moved[0] if copies == 2 else jnp.concatenate(moved, axis=0)

    peer_x = to_peers(recv[:, :width])

    (
        x_own, g_own, hidden_own, slope_own, heads, own, up_here, down_first, down_rest
    ) = pl.pallas_call(
        own_kernel,
        out_shape=(
            shape((local_count, rows, width), BF),
            shape((local_count, rows, width), BF),
            shape((local_count, rows, hidden_count), BF),
            shape((local_count, rows, hidden_count), F32),
            pltpu.VMEM((3, width, lanes), BF),
            shape((pixels, count), F32),
            pltpu.VMEM(w_up.shape, BF),
            pltpu.VMEM(w_down.shape[1:], BF),
            pltpu.VMEM((local_count - 1,) + w_down.shape[1:], BF),
        ),
        in_specs=[VMEM, HBM, HBM, HBM, HBM],
        out_specs=(VMEM,) * 9,
        scratch_shapes=[
            pltpu.VMEM(head.shape, F32),
            pltpu.VMEM(tokens.shape, BF),
            pltpu.SemaphoreType.DMA((local_count, 2)),
            pltpu.SemaphoreType.DMA((2,)),
        ],
        compiler_params=limit(16),
        cost_estimate=pl.CostEstimate(
            flops=4 * one_product,
            bytes_accessed=4 * width * hidden_count * local_count,
            transcendentals=0,
        ),
        name="own_rows",
    )(recv, w_up, w_down, stay(head), stay(tokens))

    recv_g, heads = lax.optimization_barrier((recv[:, width:], heads))
    peer_g = to_peers(recv_g)
    peer_x, heads = lax.optimization_barrier((peer_x, heads))
    others = rows * (copies - 1)
    x_peer, hidden_peer, slope_peer, scores = pl.pallas_call(
        functools.partial(peer_kernel, copies),
        out_shape=(
            shape((local_count, others, width), BF),
            shape((local_count, others, hidden_count), BF),
            shape((local_count, others, hidden_count), F32),
            shape((sources, lanes), F32),
        ),
        in_specs=[VMEM] * 6,
        out_specs=(VMEM,) * 4,
        compiler_params=limit(16),
        cost_estimate=pl.CostEstimate(flops=2 * one_product, bytes_accessed=0, transcendentals=0),
        name="peer_rows",
    )(peer_x, up_here, down_first, down_rest, heads, hidden_own)

    returned = lax.all_to_all(
        scores.reshape(sources, 1, lanes),
        ("dp", "expert"),
        split_axis=0,
        concat_axis=0,
        tiled=True,
    ).reshape(sources, lanes)

    blocks = update_blocks(local_count, width, hidden_count)
    up_tile, down_tile = [max(b[3] for b in blocks if b[1] == down) for down in (False, True)]
    updates = pl.pallas_call(
        functools.partial(update_kernel, copies),
        out_shape=(up_shape, down_shape, up_shape, up_shape, down_shape, down_shape),
        in_specs=[VMEM] * 8 + [HBM] * 6,
        out_specs=(HBM,) * 6,
        scratch_shapes=[
            pltpu.VMEM((3,) + w_up.shape, BF),
            pltpu.VMEM((3,) + w_down.shape, BF),
            pltpu.VMEM((local_count, width, rows * copies), BF),
            pltpu.VMEM((local_count, rows * copies, width), BF),
            pltpu.VMEM((local_count, rows * copies, hidden_count), BF),
            pltpu.VMEM((2, up_tile, hidden_count), F32),
            pltpu.VMEM((2, down_tile, width), F32),
            pltpu.SemaphoreType.DMA((2, len(blocks), 3)),
        ],
        compiler_params=limit(28),
        cost_estimate=pl.CostEstimate(
            flops=6 * one_product * copies,
            bytes_accessed=24 * width * hidden_count * local_count,
            transcendentals=0,
        ),
        name="update",
    )(
        x_own,
        x_peer,
        g_own,
        peer_g,
        hidden_own,
        hidden_peer,
        slope_own,
        slope_peer,
        w_up,
        w_down,
        up_moment,
        up_square,
        down_moment,
        down_square,
    )

    returned, updates = lax.optimization_barrier((returned, updates))
    fine = pl.pallas_call(
        functools.partial(finish_kernel, holders),
        out_shape=shape((pixels, count), F32),
        in_specs=[VMEM] * 4,
        out_specs=VMEM,
        compiler_params=limit(2),
        name="finish",
    )(slot, returned, own, mass.reshape(1, count))
    return (fine.T,) + tuple(updates)


def solution(mesh):
    tokens = P(("dp", "expert"), None)
    up = P("expert", None, "dp")
    down = P("expert", "dp", None)
    return jax.shard_map(
        local,
        mesh=mesh,
        in_specs=(tokens, tokens, tokens, P(), P(("dp", "expert")), P())
        + (up, down, up, up, down, down),
        out_specs=(tokens, up, down, up, up, down, down),
        check_vma=False,
    )
```
